768 devices in a mesh: blk: 96 (over y, z_lo, x), grp: 8 (over z_hi, core).
Axes of the slice: x: 4, y: 8, z: 12 (z_hi: 4, z_lo: 3; z = z_hi * 3 + z_lo), core: 2. Of those that a mesh axis runs over, the one named last changes fastest.
Arguments:
- tokens: bfloat16 [98304, 4096], P(('blk', 'grp')), may hold values from -6 to 6
- select: int32 [8, 192], P('grp', 'blk'), may hold values from 0 to 98303, as said below
- gates: float32 [8, 192], P('grp', 'blk'), may hold values from 0.1 to 1
- gate_proj: bfloat16 [8, 10752, 4096], P('grp', 'blk'), may hold values from -0.09375 to 0.09375
- up_proj: bfloat16 [8, 10752, 4096], P('grp', 'blk'), may hold values from -0.09375 to 0.09375
- down_proj: bfloat16 [8, 10752, 4096], P('grp', 'blk'), may hold values from -0.0625 to 0.0625
Outputs:
- mixed: bfloat16 [98304, 4096], P(('blk', 'grp'))
The draws below stay inside these ranges and needn't reach their ends.
Inputs may be any that keep to these rules, and one draw needn't show every extreme that they name: `select`: for every expert and every k, the slots k * 2 to (k + 1) * 2 - 1 name 2 different tokens, all from k * 8 * 128 to (k + 1) * 8 * 128 - 1.
All inputs are finite; a program needn't handle non-finite values.
Results may differ from the reference program's by a relative error of at most 0.0095.
Values may be sent and summed in bfloat16 or wider, within the bound.
A program may use at most 32 MiB of HBM per device.

```python
import math
import jax
import jax.numpy as jnp
from jax import lax

D = 4096
HID_TOTAL = 10752
EXP = 8
TOK_DEV = 128
SLOT = 2
CAP = 192
TOKENS = 98304
N_BLK = 96
N_GRP = 8


def draw_select(key, part):
    span = N_GRP * TOK_DEV
    keys = jax.random.split(jax.random.fold_in(key, 17), EXP * N_BLK)
    chosen = jax.vmap(lambda sub: jax.random.permutation(sub, span)[:SLOT])(keys)
    offsets = jnp.arange(EXP * N_BLK, dtype=jnp.int32) % N_BLK * span
    return (chosen.astype(jnp.int32) + offsets[:, None]).reshape(EXP, N_BLK * SLOT).astype(jnp.int32)


def block_levels(rng, extent, cuts, low, top_value):
    def one(position, blocks):
        steps = jax.random.uniform(jax.random.fold_in(jax.random.fold_in(rng, 6), position), (blocks,), jnp.float32, low / len(cuts), top_value / len(cuts))
        return jnp.repeat(jnp.exp(steps), extent[position] // blocks).reshape((-1,) + (1,) * (len(extent) - position - 1))

    level = one(*cuts[0])
    for cut in cuts[1:]:
        level = level * one(*cut)
    return level


def normal_values(stream_key, dims, scale, bound, cuts=(), held_as=jnp.bfloat16):
    result = jax.random.normal(stream_key, dims, jnp.float32) * scale
    if len(cuts) > 0:
        result = block_levels(stream_key, dims, cuts, -0.22, 0.18) * result
    return jnp.clip(result, min=-bound, max=bound).astype(held_as)


def setup_inputs(seed: int = 0) -> dict:
    streams_of = jax.random.split(jax.random.key(seed), 7)
    return {
        "tokens": normal_values(streams_of[0], (TOKENS, D), 1.0, 6.0, ((0, 768),)),
        "select": draw_select(jax.random.fold_in(streams_of[6], 71), 0),
        "gates": jnp.clip(jnp.exp(math.log(1.0) - 2.3025851 * jax.random.uniform(streams_of[2], (EXP, CAP), jnp.float32) ** block_levels(streams_of[2], (EXP, CAP), ((0, 8), (1, 96)), -0.2, 0.2)), 0.1, 1.0),
        "gate_proj": normal_values(streams_of[3], (EXP, HID_TOTAL, D), D ** -0.5, 0.09375, ((0, 8), (1, 96))),
        "up_proj": normal_values(streams_of[4], (EXP, HID_TOTAL, D), D ** -0.5, 0.09375, ((0, 8), (1, 96))),
        "down_proj": normal_values(streams_of[5], (EXP, HID_TOTAL, D), HID_TOTAL ** -0.5, 0.0625, ((0, 8), (1, 96))),
    }


def run_expert(operands):
    rows, w_gate, w_up, w_down = operands
    gate_act = jnp.dot(rows, w_gate.T, preferred_element_type=jnp.float32)
    up_act = jnp.dot(rows, w_up.T, preferred_element_type=jnp.float32)
    hidden = (jax.nn.silu(gate_act) * up_act).astype(jnp.bfloat16)
    return jnp.dot(hidden, w_down, preferred_element_type=jnp.float32).astype(jnp.bfloat16)


def reference(tokens, select, gates, gate_proj, up_proj, down_proj):
    picked = tokens[select.astype(jnp.int32)]
    expert_out = lax.map(run_expert, (picked, gate_proj, up_proj, down_proj))
    weighted = (gates[:, :, None] * expert_out.astype(jnp.float32)).astype(jnp.bfloat16)
    flat_ids = select.reshape(-1).astype(jnp.int32)
    mixed = jnp.zeros((TOKENS, D), jnp.float32).at[flat_ids].add(weighted.reshape(-1, D).astype(jnp.float32))
    return mixed.astype(jnp.bfloat16)
```

```python
import functools

import jax
import jax.numpy as jnp
import numpy as np
from jax import lax
from jax.experimental import pallas as pl
from jax.experimental.pallas import tpu as pltpu
from jax.sharding import Mesh
from jax.sharding import PartitionSpec as P

BLK = ("y", "z", "x")
BLK_GRP = ("y", "z", "x", "grp")
NY, NZ, NX = 8, 3, 4
YC, XC = 3, 3
YR, XR = NX * NZ * 2 // YC, NY * NZ * 2 // XC


def remote(src, dst, send_sem, recv_sem, **where):
    return pltpu.make_async_remote_copy(
        src_ref=src,
        dst_ref=dst,
        send_sem=send_sem,
        recv_sem=recv_sem,
        device_id=where,
        device_id_type=pl.DeviceIdType.MESH,
    )


def turn(index, by, size):
    return lax.rem(index + by + size, size)


def experts_kernel(
    picked,
    w_gate_hbm,
    w_up_hbm,
    w_down_hbm,
    perm,
    perm_t,
    out,
    w_gate,
    w_up,
    w_down,
    z_rows,
    x_rows,
    y_rows,
    rows_f32,
    ring_y,
    ring_x,
    part_y,
    part_x,
    send_y,
    send_x,
    recv_y,
    recv_x,
    flat_f32,
    mid_x_f32,
    mid_x,
    mid_x_recv,
    mid_y_f32,
    mid_y,
    mid_y_recv,
    mid_z_f32,
    mid_z,
    mid_z_recv,
    w_sem,
    gz_send,
    gz_recv,
    gx_send,
    gx_recv,
    gy_send,
    gy_recv,
    gry_send,
    gry_recv,
    grx_send,
    grx_recv,
    sry_send,
    sry_recv,
    srx_send,
    srx_recv,
    sx_send,
    sx_recv,
    sy_send,
    sy_recv,
    sz_send,
    sz_recv,
):
    y, z, x = lax.axis_index("y"), lax.axis_index("z"), lax.axis_index("x")
    width = picked.shape[-1]
    half = width // 2
    quarter = half // 2
    f32, bf16 = jnp.float32, jnp.bfloat16
    sent = []

    weights = [
        pltpu.make_async_copy(src.at[0], dst, w_sem.at[k])
        for k, (src, dst) in enumerate(
            ((w_gate_hbm, w_gate), (w_up_hbm, w_up), (w_down_hbm, w_down))
        )
    ]
    for copy in weights:
        copy.start()

    barrier = pltpu.get_barrier_semaphore()
    for o in range(1, NZ):
        pl.semaphore_signal(barrier, device_id={"z": turn(z, o, NZ)})
    for o in range(1, NX):
        pl.semaphore_signal(barrier, device_id={"x": turn(x, o, NX)})
    for o in range(1, NY):
        pl.semaphore_signal(barrier, device_id={"y": turn(y, o, NY)})
    pl.semaphore_wait(barrier, NZ + NX + NY - 3)

    def go(copy):
        copy.start()
        sent.append(copy)

    for o in range(1, NZ):
        go(remote(picked.at[0], z_rows.at[z], gz_send.at[o - 1], gz_recv.at[o - 1], z=turn(z, o, NZ)))
    z_rows[z] = picked[0]
    for o in range(1, NZ):
        landed = z_rows.at[turn(z, -o, NZ)]
        remote(landed, landed, gz_send.at[o - 1], gz_recv.at[o - 1], z=turn(z, o, NZ)).wait_recv()

    for o in range(1, NX):
        go(
            remote(
                z_rows.at[:, :, :half],
                x_rows.at[x],
                gx_send.at[o - 1],
                gx_recv.at[o - 1],
                x=turn(x, o, NX),
            )
        )
    for o in range(1, NY):
        go(
            remote(
                z_rows.at[:, :, half:],
                y_rows.at[y],
                gy_send.at[o - 1],
                gy_recv.at[o - 1],
                y=turn(y, o, NY),
            )
        )
    x_rows[x] = z_rows[:, :, :half]
    y_rows[y] = z_rows[:, :, half:]

    def ring_gather(axis, me, size, chunks, buf, sems, recvs):
        steps = size // 2

        def part(block, c, hop, way):
            ref = buf.at[block * chunks + c]
            if hop == steps:
                ref = ref.at[:, :quarter] if way == 0 else ref.at[:, quarter:]
            return ref

        def send(hop, way, c):
            sign = 1 - 2 * way
            ref = part(turn(me, -sign * (hop - 1), size), c, hop, way)
            at = ((hop - 1) * 2 + way) * chunks + c
            go(remote(ref, ref, sems.at[at], recvs.at[at], **{axis: turn(me, sign, size)}))

        def wait(hop, way, c):
            sign = 1 - 2 * way
            ref = part(turn(me, -sign * hop, size), c, hop, way)
            at = ((hop - 1) * 2 + way) * chunks + c
            remote(ref, ref, sems.at[at], recvs.at[at], **{axis: turn(me, sign, size)}).wait_recv()

        return send, wait

    def each(count):
        return [(c, way) for c in range(count) for way in range(2)]

    y_send, y_wait = ring_gather("y", y, NY, YC, ring_y, gry_send, gry_recv)
    x_send, x_wait = ring_gather("x", x, NX, XC, ring_x, grx_send, grx_recv)

    for o in range(1, NX):
        landed = x_rows.at[turn(x, -o, NX)]
        remote(landed, landed, gx_send.at[o - 1], gx_recv.at[o - 1], x=turn(x, o, NX)).wait_recv()
    for i in range(NX):
        for j in range(NZ):
            rows_f32[pl.ds((i * NZ + j) * 2, 2), :] = x_rows[i, j].astype(f32)
    for c in range(YC):
        ring_y[y * YC + c] = rows_f32[pl.ds(c * YR, YR), :].astype(bf16)
    for c, way in each(YC):
        y_send(1, way, c)

    for o in range(1, NY):
        landed = y_rows.at[turn(y, -o, NY)]
        remote(landed, landed, gy_send.at[o - 1], gy_recv.at[o - 1], y=turn(y, o, NY)).wait_recv()
    for i in range(NY):
        for j in range(NZ):
            rows_f32[pl.ds((i * NZ + j) * 2, 2), :] = y_rows[i, j].astype(f32)
    for c in range(XC):
        ring_x[x * XC + c] = rows_f32[pl.ds(c * XR, XR), :].astype(bf16)
    for c, way in each(XC):
        x_send(1, way, c)

    for c, way in each(YC):
        y_wait(1, way, c)
        y_send(2, way, c)
    for c, way in each(YC):
        y_wait(2, way, c)
        y_send(3, way, c)
        x_wait(1, way, c)
        x_send(2, way, c)
    for c, way in each(YC):
        y_wait(3, way, c)
        y_send(4, way, c)
    for c, way in each(XC):
        x_wait(2, way, c)
    for c, way in each(YC):
        y_wait(4, way, c)

    for copy in weights:
        copy.wait()
    rows_all = NX * NY * NZ * 2
    dims = (((1,), (1,)), ((), ()))

    def rows_of(ref):
        return ref[...].astype(f32).reshape(rows_all, half).astype(bf16)

    right = rows_of(ring_x)
    gate_r = lax.dot_general(right, w_gate[:, half:], dims, preferred_element_type=f32)
    up_r = lax.dot_general(right, w_up[:, half:], dims, preferred_element_type=f32)
    turned = perm[...].astype(f32)
    gate_r = jnp.dot(turned, gate_r, preferred_element_type=f32, precision=lax.Precision.HIGHEST)
    up_r = jnp.dot(turned, up_r, preferred_element_type=f32, precision=lax.Precision.HIGHEST)
    left = rows_of(ring_y)
    gate_act = gate_r + lax.dot_general(left, w_gate[:, :half], dims, preferred_element_type=f32)
    up_act = up_r + lax.dot_general(left, w_up[:, :half], dims, preferred_element_type=f32)
    hidden = (gate_act / (1.0 + jnp.exp(-gate_act)) * up_act).astype(bf16)
    hidden_t = jnp.dot(perm_t[...], hidden, preferred_element_type=f32).astype(bf16)

    def ring_sum(axis, me, size, chunks, parts, buf, landed, sems, recvs):
        steps = size // 2

        def cut(ref, hop, way):
            if hop == 1:
                ref = ref.at[:, :quarter] if way == 0 else ref.at[:, quarter:]
            return ref

        def copy(hop, way, c):
            sign = 1 - 2 * way
            at = ((hop - 1) * 2 + way) * chunks + c
            dest = turn(me, sign * (steps + 1 - hop), size)
            return remote(
                cut(buf.at[dest * chunks + c], hop, way),
                cut(landed.at[at], hop, way),
                sems.at[at],
                recvs.at[at],
                **{axis: turn(me, sign, size)},
            )

        def first(c):
            at = turn(me, steps, size) * chunks + c
            buf[at] = parts[at].astype(bf16)
            for way in range(2):
                go(copy(1, way, c))

        def add(hop, way, c):
            copy(hop, way, c).wait_recv()
            sign = 1 - 2 * way
            at = turn(me, sign * (steps - hop), size) * chunks + c
            got = landed.at[((hop - 1) * 2 + way) * chunks + c]
            if hop == 1:
                mine, other = (slice(0, quarter), slice(quarter, half))[:: 1 - 2 * way]
                buf[at, :, mine] = (parts[at, :, mine] + got[:, mine].astype(f32)).astype(bf16)
                buf[at, :, other] = parts[at, :, other].astype(bf16)
            else:
                buf[at] = (parts[at] + got[...].astype(f32)).astype(bf16)
            go(copy(hop + 1, way, c))

        def last(c):
            total = parts[me * chunks + c]
            for way in range(2):
                copy(steps, way, c).wait_recv()
                total = total + landed[((steps - 1) * 2 + way) * chunks + c].astype(f32)
            return total

        return first, add, last

    y_first, y_add, y_last = ring_sum(
        "y", y, NY, YC, part_y, send_y, recv_y, sry_send, sry_recv
    )
    x_first, x_add, x_last = ring_sum(
        "x", x, NX, XC, part_x, send_x, recv_x, srx_send, srx_recv
    )

    part_y[...] = jnp.dot(hidden, w_down[:, :half], preferred_element_type=f32).reshape(part_y.shape)
    for c in range(YC):
        y_first(c)
    part_x[...] = jnp.dot(hidden_t, w_down[:, half:], preferred_element_type=f32).reshape(part_x.shape)
    for c in range(XC):
        x_first(c)
    for c, way in each(YC):
        y_add(1, way, c)
    for c, way in each(YC):
        y_add(2, way, c)
        x_add(1, way, c)
    for c, way in each(YC):
        y_add(3, way, c)

    for c in range(XC):
        flat_f32[pl.ds(c * XR, XR), :] = x_last(c)
    for i in range(NY):
        for j in range(NZ):
            rows = flat_f32[pl.ds((i * NZ + j) * 2, 2), :]
            mid_y_f32[i, j] = rows
            mid_y[i, j] = rows.astype(bf16)
    for o in range(1, NY):
        go(
            remote(
                mid_y.at[turn(y, o, NY)],
                mid_y_recv.at[o - 1],
                sy_send.at[o - 1],
                sy_recv.at[o - 1],
                y=turn(y, o, NY),
            )
        )
    for c in range(YC):
        flat_f32[pl.ds(c * YR, YR), :] = y_last(c)
    for i in range(NX):
        for j in range(NZ):
            rows = flat_f32[pl.ds((i * NZ + j) * 2, 2), :]
            mid_x_f32[i, j] = rows
            mid_x[i, j] = rows.astype(bf16)
    for o in range(1, NX):
        go(
            remote(
                mid_x.at[turn(x, o, NX)],
                mid_x_recv.at[o - 1],
                sx_send.at[o - 1],
                sx_recv.at[o - 1],
                x=turn(x, o, NX),
            )
        )

    total = mid_y_f32[y]
    for o in range(1, NY):
        landed = mid_y_recv.at[o - 1]
        remote(landed, landed, sy_send.at[o - 1], sy_recv.at[o - 1], y=turn(y, o, NY)).wait_recv()
        total = total + landed[...].astype(f32)
    mid_z_f32[:, :, half:] = total
    mid_z[:, :, half:] = total.astype(bf16)
    total = mid_x_f32[x]
    for o in range(1, NX):
        landed = mid_x_recv.at[o - 1]
        remote(landed, landed, sx_send.at[o - 1], sx_recv.at[o - 1], x=turn(x, o, NX)).wait_recv()
        total = total + landed[...].astype(f32)
    mid_z_f32[:, :, :half] = total
    mid_z[:, :, :half] = total.astype(bf16)
    for o in range(1, NZ):
        go(
            remote(
                mid_z.at[turn(z, o, NZ)],
                mid_z_recv.at[o - 1],
                sz_send.at[o - 1],
                sz_recv.at[o - 1],
                z=turn(z, o, NZ),
            )
        )
    total = mid_z_f32[z]
    for o in range(1, NZ):
        landed = mid_z_recv.at[o - 1]
        remote(landed, landed, sz_send.at[o - 1], sz_recv.at[o - 1], z=turn(z, o, NZ)).wait_recv()
        total = total + landed[...].astype(f32)
    out[0] = total

    for copy in sent:
        copy.wait_send()


def swap_matrix():
    k = np.arange(NY * NX * NZ * 2)
    per = NZ * 2
    i, j, q = k // (per * NX), k // per % NX, k % per
    table = np.zeros((k.size, k.size), np.float32)
    table[k, (j * NY + i) * per + q] = 1
    return table


def experts(picked, w_gate, w_up, w_down):
    width = picked.shape[-1]
    half = width // 2
    bf16, f32 = jnp.bfloat16, jnp.float32
    rows = NX * NY * NZ * 2
    table = swap_matrix()
    dma = pltpu.SemaphoreType.DMA
    vmem = pltpu.VMEM
    ring = lambda n, c: n // 2 * 2 * c
    weight = vmem(w_gate.shape[1:], bf16)
    scratch = [
        weight,
        weight,
        weight,
        vmem((NZ, 2, width), bf16),
        vmem((NX, NZ, 2, half), bf16),
        vmem((NY, NZ, 2, half), bf16),
        vmem((NY * NZ * 2, half), f32),
        vmem((NY * YC, YR, half), bf16),
        vmem((NX * XC, XR, half), bf16),
        vmem((NY * YC, YR, half), f32),
        vmem((NX * XC, XR, half), f32),
        vmem((NY * YC, YR, half), bf16),
        vmem((NX * XC, XR, half), bf16),
        vmem((ring(NY, YC), YR, half), bf16),
        vmem((ring(NX, XC), XR, half), bf16),
        vmem((NY * NZ * 2, half), f32),
        vmem((NX, NZ, 2, half), f32),
        vmem((NX, NZ, 2, half), bf16),
        vmem((NX - 1, NZ, 2, half), bf16),
        vmem((NY, NZ, 2, half), f32),
        vmem((NY, NZ, 2, half), bf16),
        vmem((NY - 1, NZ, 2, half), bf16),
        vmem((NZ, 2, width), f32),
        vmem((NZ, 2, width), bf16),
        vmem((NZ - 1, 2, width), bf16),
        dma((3,)),
    ]
    for count in (NZ - 1, NX - 1, NY - 1, ring(NY, YC), ring(NX, XC), ring(NY, YC), ring(NX, XC), NX - 1, NY - 1, NZ - 1):
        scratch += [dma((count,)), dma((count,))]
    in_vmem = pl.BlockSpec(memory_space=pltpu.VMEM)
    in_hbm = pl.BlockSpec(memory_space=pl.ANY)
    return pl.pallas_call(
        experts_kernel,
        out_shape=jax.ShapeDtypeStruct((1, 2, width), f32),
        in_specs=[in_vmem, in_hbm, in_hbm, in_hbm, in_vmem, in_vmem],
        out_specs=in_vmem,
        scratch_shapes=scratch,
        compiler_params=pltpu.CompilerParams(
            collective_id=0, has_side_effects=True, vmem_limit_bytes=56 * 1024 * 1024
        ),
        name="experts",
    )(
        picked,
        w_gate,
        w_up,
        w_down,
        jnp.asarray(table, bf16),
        jnp.asarray(table.T, bf16),
    )


def sent_to_all(array, axis):
    copies = jnp.broadcast_to(array, (lax.axis_size(axis), *array.shape))
    return lax.all_to_all(copies, axis, split_axis=0, concat_axis=0, tiled=True)


def collect(array, axis):
    blocks = sent_to_all(array, axis)
    return blocks.reshape(-1, *array.shape[1:])


def on_device(tokens, select, gates, gate_proj, up_proj, down_proj):
    groups = lax.axis_size("grp")
    tok_dev, width = tokens.shape
    slots = select.shape[1]
    first = (lax.axis_index(BLK) * groups + lax.axis_index("grp")) * tok_dev
    local_ids = collect(select, "grp").reshape(-1) - first
    owned = (local_ids[:, None] == jnp.arange(tok_dev, dtype=jnp.int32)[None, :]).astype(
        jnp.bfloat16
    )
    candidates = jnp.dot(owned, tokens, preferred_element_type=jnp.float32)
    arrived = lax.all_to_all(
        candidates.astype(jnp.bfloat16), "grp", split_axis=0, concat_axis=0, tiled=True
    )
    picked = jnp.sum(arrived.reshape(groups, slots, width).astype(jnp.float32), axis=0).astype(
        jnp.bfloat16
    )
    summed = experts(picked[None], gate_proj, up_proj, down_proj)[0]
    expert_out = summed.astype(jnp.bfloat16)
    weighted = (gates[0][:, None] * expert_out.astype(jnp.float32)).astype(jnp.bfloat16)
    mixed = jnp.dot(owned.T, collect(weighted, "grp"), preferred_element_type=jnp.float32)
    return mixed.astype(jnp.bfloat16)


def solution(mesh):
    finer = Mesh(mesh.devices.reshape(NY, NZ, NX, mesh.shape["grp"]), BLK_GRP)
    in_specs = (
        P(BLK_GRP, None),
        P("grp", BLK),
        P("grp", BLK),
        P("grp", BLK, None),
        P("grp", BLK, None),
        P("grp", BLK, None),
    )
    return jax.shard_map(
        on_device, mesh=finer, in_specs=in_specs, out_specs=P(BLK_GRP, None), check_vma=False
    )
```

```python
import jax
import jax.numpy as jnp
import numpy as np
from jax import lax
from jax.experimental import pallas as pl
from jax.experimental.pallas import tpu as pltpu
from jax.sharding import Mesh
from jax.sharding import PartitionSpec as P

BLK = ("y", "z", "x")
BLK_GRP = ("y", "z", "x", "grp")
NY, NZ, NX = 8, 3, 4
NH, NC = 4, 2
NG = NH * NC
YC, XC = 3, 3
YR, XR = NX * NZ * 2 // YC, NY * NZ * 2 // XC
ROWS = NX * NY * NZ * 2
FAR_FIRST = [(h, c) for h in (2, 1, 3, 0) for c in range(NC) if h or c]
LEFT, RIGHT = 0, 1


def remote(src, dst, send_sem, recv_sem, **where):
    return pltpu.make_async_remote_copy(
        src_ref=src,
        dst_ref=dst,
        send_sem=send_sem,
        recv_sem=recv_sem,
        device_id=where,
        device_id_type=pl.DeviceIdType.MESH,
    )


def turn(index, by, size):
    return lax.rem(index + by + size, size)


def each(count):
    return [(c, way) for c in range(count) for way in range(2)]


def ring_gather(go, axis, me, size, chunks, buf, sems, recvs):
    steps = size // 2
    middle = buf.shape[-1] // 2

    def copy(block, hop, way, c):
        ref = buf.at[block * chunks + c]
        if hop == steps:
            ref = ref.at[:, :middle] if way == 0 else ref.at[:, middle:]
        at = ((hop - 1) * 2 + way) * chunks + c
        return remote(ref, ref, sems.at[at], recvs.at[at], **{axis: turn(me, 1 - 2 * way, size)})

    def send(hop, way, c):
        go(copy(turn(me, (2 * way - 1) * (hop - 1), size), hop, way, c))

    def wait(hop, way, c):
        copy(turn(me, (2 * way - 1) * hop, size), hop, way, c).wait_recv()

    return send, wait


def ring_sum(go, axis, me, size, chunks, parts, buf, landed, sems, recvs):
    steps = size // 2
    half = buf.shape[-1]
    middle = half // 2
    f32, bf16 = jnp.float32, jnp.bfloat16

    def cut(ref, hop, way):
        if hop == 1:
            ref = ref.at[:, :middle] if way == 0 else ref.at[:, middle:]
        return ref

    def copy(hop, way, c):
        sign = 1 - 2 * way
        at = ((hop - 1) * 2 + way) * chunks + c
        dest = turn(me, sign * (steps + 1 - hop), size)
        return remote(
            cut(buf.at[dest * chunks + c], hop, way),
            cut(landed.at[at], hop, way),
            sems.at[at],
            recvs.at[at],
            **{axis: turn(me, sign, size)},
        )

    def first(c):
        at = turn(me, steps, size) * chunks + c
        buf[at] = parts[at].astype(bf16)
        for way in range(2):
            go(copy(1, way, c))

    def add(hop, way, c):
        copy(hop, way, c).wait_recv()
        at = turn(me, (1 - 2 * way) * (steps - hop), size) * chunks + c
        got = landed.at[((hop - 1) * 2 + way) * chunks + c]
        if hop == 1:
            mine, other = (slice(0, middle), slice(middle, half))[:: 1 - 2 * way]
            buf[at, :, mine] = (parts[at, :, mine] + got[:, mine].astype(f32)).astype(bf16)
            buf[at, :, other] = parts[at, :, other].astype(bf16)
        else:
            buf[at] = (parts[at] + got[...].astype(f32)).astype(bf16)
        go(copy(hop + 1, way, c))

    def last(c):
        total = parts[me * chunks + c]
        for way in range(2):
            copy(steps, way, c).wait_recv()
            total = total + landed[((steps - 1) * 2 + way) * chunks + c].astype(f32)
        return total

    return first, add, last


def layer_kernel(
    ids,
    gates,
    perm,
    perm_t,
    tokens_hbm,
    gate_hbm,
    up_hbm,
    down_hbm,
    rows_out,
    owned_out,
    tokens,
    w_in,
    w_out,
    all_ids,
    owned,
    cand_f32,
    cand,
    arrived,
    z_rows,
    x_rows,
    y_rows,
    flat_f32,
    ring_y,
    ring_x,
    part_y,
    part_x,
    sum_y,
    sum_x,
    got_y,
    got_x,
    mid_x_f32,
    mid_x,
    mid_x_got,
    mid_y_f32,
    mid_y,
    mid_y_got,
    mid_z,
    mid_z_got,
    weighted,
    gathered,
    w_sem,
    *sems,
):
    y, z, x = lax.axis_index("y"), lax.axis_index("z"), lax.axis_index("x")
    g = lax.axis_index("grp")
    chip, core = g // NC, lax.rem(g, NC)
    tok_dev, width = tokens.shape
    half = width // 2
    hid = gate_hbm.shape[1]
    pad = w_out.shape[0]
    cols = (slice(0, half), slice(half, width))
    f32, bf16 = jnp.float32, jnp.bfloat16
    (
        (id_send, id_recv),
        (row_send, row_recv),
        (gz_send, gz_recv),
        (gx_send, gx_recv),
        (gy_send, gy_recv),
        ring_gy,
        ring_gx,
        ring_sy,
        ring_sx,
        (sx_send, sx_recv),
        (sy_send, sy_recv),
        (sz_send, sz_recv),
        (out_send, out_recv),
    ) = zip(sems[::2], sems[1::2])
    sent = []

    def go(copy):
        copy.start()
        sent.append(copy)

    def peer(h, c, sign=1):
        return turn(chip, sign * h, NH) * NC + turn(core, sign * c, NC)

    loads = [
        pltpu.make_async_copy(tokens_hbm, tokens, w_sem.at[0]),
        pltpu.make_async_copy(gate_hbm.at[0], w_in.at[pl.ds(0, hid)], w_sem.at[1]),
        pltpu.make_async_copy(up_hbm.at[0], w_in.at[pl.ds(pad, hid)], w_sem.at[2]),
        pltpu.make_async_copy(down_hbm.at[0], w_out.at[pl.ds(0, hid)], w_sem.at[3]),
    ]
    for copy in loads:
        copy.start()

    barrier = pltpu.get_barrier_semaphore()
    for h, c in FAR_FIRST:
        pl.semaphore_signal(barrier, device_id={"grp": peer(h, c)})
    for o in range(1, NY):
        pl.semaphore_signal(barrier, device_id={"y": turn(y, o, NY)})
    for o in range(1, NX):
        pl.semaphore_signal(barrier, device_id={"x": turn(x, o, NX)})
    for o in range(1, NZ):
        pl.semaphore_signal(barrier, device_id={"z": turn(z, o, NZ)})
    pl.semaphore_wait(barrier, NG + NZ + NX + NY - 4)

    for h, c in FAR_FIRST:
        at = h * NC + c
        go(remote(ids, all_ids.at[g], id_send.at[at], id_recv.at[at], grp=peer(h, c)))
    all_ids[g] = ids[...]
    for at in (hid, pad + hid):
        w_in[pl.ds(at, pad - hid), :] = jnp.zeros((pad - hid, width), bf16)
    w_out[pl.ds(hid, pad - hid), :] = jnp.zeros((pad - hid, width), bf16)
    loads[0].wait()
    for h, c in FAR_FIRST[::-1]:
        at, landed = h * NC + c, all_ids.at[peer(h, c, -1)]
        remote(landed, landed, id_send.at[at], id_recv.at[at], grp=peer(h, c)).wait_recv()

    block = (y * NZ + z) * NX + x
    lane = lax.broadcasted_iota(jnp.int32, (2, tok_dev), 1) + (block * NG + g) * tok_dev
    for e in range(NG):
        owned[pl.ds(e * 2, 2), :] = (all_ids[e] == lane).astype(f32)
    chosen = owned[...].astype(bf16)
    for k in (RIGHT, LEFT):
        cand_f32[...] = jnp.dot(chosen, tokens[:, cols[k]], preferred_element_type=f32)
        for e in range(NG):
            cand[k, e] = cand_f32[pl.ds(e * 2, 2), :].astype(bf16)
        for h, c in FAR_FIRST:
            at, to = h * NC + c, peer(h, c)
            go(
                remote(
                    cand.at[k, to],
                    arrived.at[k, at],
                    row_send.at[k * NG + at],
                    row_recv.at[k * NG + at],
                    grp=to,
                )
            )

    def spread(k, o):
        src = z_rows.at[k, turn(z, -o, NZ)]
        axis, me, size, buf, send, recv = (
            ("x", x, NX, x_rows, gx_send, gx_recv),
            ("y", y, NY, y_rows, gy_send, gy_recv),
        )[k]
        for d in range(1, size):
            at = o * (size - 1) + d - 1
            dst = buf.at[me, turn(z, -o, NZ)]
            go(remote(src, dst, send.at[at], recv.at[at], **{axis: turn(me, d, size)}))
        buf[me, turn(z, -o, NZ)] = src[...]

    def spread_wait(k):
        axis, me, size, buf, send, recv = (
            ("x", x, NX, x_rows, gx_send, gx_recv),
            ("y", y, NY, y_rows, gy_send, gy_recv),
        )[k]
        for o in range(NZ):
            for d in range(1, size):
                at = o * (size - 1) + d - 1
                landed = buf.at[turn(me, -d, size), turn(z, -o, NZ)]
                remote(
                    landed, landed, send.at[at], recv.at[at], **{axis: turn(me, d, size)}
                ).wait_recv()

    for k in (RIGHT, LEFT):
        total = cand[k, g].astype(f32)
        for h, c in FAR_FIRST[::-1]:
            at = h * NC + c
            landed = arrived.at[k, at]
            remote(
                landed, landed, row_send.at[k * NG + at], row_recv.at[k * NG + at], grp=peer(h, c)
            ).wait_recv()
            total = total + landed[...].astype(f32)
        z_rows[k, z] = total.astype(bf16)
        for o in range(1, NZ):
            at = k * (NZ - 1) + o - 1
            ref = z_rows.at[k, z]
            go(remote(ref, ref, gz_send.at[at], gz_recv.at[at], z=turn(z, o, NZ)))
        spread(k, 0)
    for k in (RIGHT, LEFT):
        for o in range(1, NZ):
            at = k * (NZ - 1) + o - 1
            landed = z_rows.at[k, turn(z, -o, NZ)]
            remote(landed, landed, gz_send.at[at], gz_recv.at[at], z=turn(z, o, NZ)).wait_recv()
            spread(k, o)

    y_send, y_wait = ring_gather(go, "y", y, NY, YC, ring_y, *ring_gy)
    x_send, x_wait = ring_gather(go, "x", x, NX, XC, ring_x, *ring_gx)

    spread_wait(LEFT)
    for i in range(NX):
        for j in range(NZ):
            flat_f32[pl.ds((i * NZ + j) * 2, 2), :] = x_rows[i, j].astype(f32)
    for c in range(YC):
        ring_y[y * YC + c] = flat_f32[pl.ds(c * YR, YR), :].astype(bf16)
    for c, way in each(YC):
        y_send(1, way, c)
    spread_wait(RIGHT)
    for i in range(NY):
        for j in range(NZ):
            flat_f32[pl.ds((i * NZ + j) * 2, 2), :] = y_rows[i, j].astype(f32)
    for c in range(XC):
        ring_x[x * XC + c] = flat_f32[pl.ds(c * XR, XR), :].astype(bf16)
    for c, way in each(XC):
        x_send(1, way, c)
    for c, way in each(YC):
        y_wait(1, way, c)
        y_send(2, way, c)
    for c, way in each(YC):
        y_wait(2, way, c)
        y_send(3, way, c)
        x_wait(1, way, c)
        x_send(2, way, c)
    for c, way in each(YC):
        y_wait(3, way, c)
        y_send(4, way, c)
    for copy in loads[1:]:
        copy.wait()
    for c, way in each(XC):
        x_wait(2, way, c)

    def from_ring(ref, k):
        rows = ref[...].astype(f32).reshape(ROWS, half).astype(bf16)
        return lax.dot_general(
            rows, w_in[:, cols[k]], (((1,), (1,)), ((), ())), preferred_element_type=f32
        )

    act = from_ring(ring_x, RIGHT)
    high = act.astype(bf16)
    rest = act - high.astype(f32)
    middle = rest.astype(bf16)
    low = (rest - middle.astype(f32)).astype(bf16)
    act = sum(jnp.dot(perm[...], term, preferred_element_type=f32) for term in (low, middle, high))
    for c, way in each(YC):
        y_wait(4, way, c)
    act = act + from_ring(ring_y, LEFT)
    gate_act, up_act = act[:, :pad], act[:, pad:]
    hidden = (gate_act / (1.0 + jnp.exp(-gate_act)) * up_act).astype(bf16)

    y_first, y_add, y_last = ring_sum(go, "y", y, NY, YC, part_y, sum_y, got_y, *ring_sy)
    x_first, x_add, x_last = ring_sum(go, "x", x, NX, XC, part_x, sum_x, got_x, *ring_sx)

    part_y[...] = jnp.dot(hidden, w_out[:, :half], preferred_element_type=f32).reshape(part_y.shape)
    for c in range(YC):
        y_first(c)
    hidden_t = jnp.dot(perm_t[...], hidden, preferred_element_type=f32).astype(bf16)
    part_x[...] = jnp.dot(hidden_t, w_out[:, half:], preferred_element_type=f32).reshape(part_x.shape)
    for c in range(XC):
        x_first(c)
    for c, way in each(YC):
        y_add(1, way, c)
    for c, way in each(YC):
        y_add(2, way, c)
        x_add(1, way, c)
    for c, way in each(YC):
        y_add(3, way, c)

    mids = (
        ("x", x, NX, mid_x_f32, mid_x, mid_x_got, sx_send, sx_recv),
        ("y", y, NY, mid_y_f32, mid_y, mid_y_got, sy_send, sy_recv),
    )

    def back(k, last, chunks, height):
        axis, me, size, wide, buf, got, send, recv = mids[k]
        for c in range(chunks):
            flat_f32[pl.ds(c * height, height), :] = last(c)
        for i in range(size):
            for j in range(NZ):
                rows = flat_f32[pl.ds((i * NZ + j) * 2, 2), :]
                wide[i, j] = rows
                buf[i, j] = rows.astype(bf16)
        for o in (1, 2, 0):
            for d in range(1, size):
                at = o * (size - 1) + d - 1
                src = buf.at[turn(me, d, size), turn(z, o, NZ)]
                go(remote(src, got.at[at], send.at[at], recv.at[at], **{axis: turn(me, d, size)}))

    def back_sum(k, o):
        axis, me, size, wide, buf, got, send, recv = mids[k]
        total = wide[me, turn(z, o, NZ)]
        for d in range(1, size):
            at = o * (size - 1) + d - 1
            landed = got.at[at]
            remote(
                landed, landed, send.at[at], recv.at[at], **{axis: turn(me, d, size)}
            ).wait_recv()
            total = total + landed[...].astype(f32)
        return total

    back(RIGHT, x_last, XC, XR)
    back(LEFT, y_last, YC, YR)
    for k in (LEFT, RIGHT):
        for o in range(1, NZ):
            at = k * (NZ - 1) + o - 1
            mid_z[at] = back_sum(k, o).astype(bf16)
            go(
                remote(
                    mid_z.at[at], mid_z_got.at[at], sz_send.at[at], sz_recv.at[at], z=turn(z, o, NZ)
                )
            )
    for k in (LEFT, RIGHT):
        total = back_sum(k, 0)
        for o in range(1, NZ):
            at = k * (NZ - 1) + o - 1
            landed = mid_z_got.at[at]
            remote(landed, landed, sz_send.at[at], sz_recv.at[at], z=turn(z, o, NZ)).wait_recv()
            total = total + landed[...].astype(f32)
        weighted[k] = (gates[:, :1] * total.astype(bf16).astype(f32)).astype(bf16)
        for h, c in FAR_FIRST:
            at = k * NG + h * NC + c
            go(
                remote(
                    weighted.at[k], gathered.at[k, g], out_send.at[at], out_recv.at[at], grp=peer(h, c)
                )
            )
        gathered[k, g] = weighted[k]

    owned_out[...] = chosen
    for k in (LEFT, RIGHT):
        for h, c in FAR_FIRST[::-1]:
            at = k * NG + h * NC + c
            landed = gathered.at[k, peer(h, c, -1)]
            remote(landed, landed, out_send.at[at], out_recv.at[at], grp=peer(h, c)).wait_recv()
        rows_out[:, :, cols[k]] = gathered[k]
    for copy in sent:
        copy.wait_send()


def swap_matrix():
    k = np.arange(ROWS)
    per = NZ * 2
    i, j, q = k // (per * NX), k // per % NX, k % per
    table = np.zeros((ROWS, ROWS), np.float32)
    table[k, (j * NY + i) * per + q] = 1
    return table


def on_device(tokens, select, gates, gate_proj, up_proj, down_proj):
    tok_dev, width = tokens.shape
    half = width // 2
    bf16, f32 = jnp.bfloat16, jnp.float32
    dma, vmem = pltpu.SemaphoreType.DMA, pltpu.VMEM
    hops_y, hops_x = NY * YC, NX * XC
    pad = -(-gate_proj.shape[1] // 128) * 128
    scratch = [
        vmem((tok_dev, width), bf16),
        vmem((2 * pad, width), bf16),
        vmem((pad, width), bf16),
        vmem((NG, 2, tok_dev), jnp.int32),
        vmem((NG * 2, tok_dev), f32),
        vmem((NG * 2, half), f32),
        vmem((2, NG, 2, half), bf16),
        vmem((2, NG, 2, half), bf16),
        vmem((2, NZ, 2, half), bf16),
        vmem((NX, NZ, 2, half), bf16),
        vmem((NY, NZ, 2, half), bf16),
        vmem((NY * NZ * 2, half), f32),
        vmem((NY * YC, YR, half), bf16),
        vmem((NX * XC, XR, half), bf16),
        vmem((NY * YC, YR, half), f32),
        vmem((NX * XC, XR, half), f32),
        vmem((NY * YC, YR, half), bf16),
        vmem((NX * XC, XR, half), bf16),
        vmem((hops_y, YR, half), bf16),
        vmem((hops_x, XR, half), bf16),
        vmem((NX, NZ, 2, half), f32),
        vmem((NX, NZ, 2, half), bf16),
        vmem((NZ * (NX - 1), 2, half), bf16),
        vmem((NY, NZ, 2, half), f32),
        vmem((NY, NZ, 2, half), bf16),
        vmem((NZ * (NY - 1), 2, half), bf16),
        vmem((2 * (NZ - 1), 2, half), bf16),
        vmem((2 * (NZ - 1), 2, half), bf16),
        vmem((2, 2, half), bf16),
        vmem((2, NG, 2, half), bf16),
        dma((4,)),
    ]
    for count in (
        NG,
        2 * NG,
        2 * (NZ - 1),
        NZ * (NX - 1),
        NZ * (NY - 1),
        hops_y,
        hops_x,
        hops_y,
        hops_x,
        NZ * (NX - 1),
        NZ * (NY - 1),
        2 * (NZ - 1),
        2 * NG,
    ):
        scratch += [dma((count,)), dma((count,))]
    in_vmem = pl.BlockSpec(memory_space=pltpu.VMEM)
    in_hbm = pl.BlockSpec(memory_space=pl.ANY)
    table = swap_matrix()
    rows, owned = pl.pallas_call(
        layer_kernel,
        out_shape=(
            jax.ShapeDtypeStruct((NG, 2, width), bf16),
            jax.ShapeDtypeStruct((NG * 2, tok_dev), bf16),
        ),
        in_specs=[in_vmem] * 4 + [in_hbm] * 4,
        out_specs=(in_vmem, in_vmem),
        scratch_shapes=scratch,
        compiler_params=pltpu.CompilerParams(
            collective_id=0, has_side_effects=True, vmem_limit_bytes=56 * 1024 * 1024
        ),
        name="layer",
    )(
        jnp.broadcast_to(select.reshape(2, 1), (2, tok_dev)),
        jnp.broadcast_to(gates.reshape(2, 1), (2, 128)),
        jnp.asarray(table, bf16),
        jnp.asarray(table.T, bf16),
        tokens,
        gate_proj,
        up_proj,
        down_proj,
    )
    mixed = jnp.dot(owned.T, rows.reshape(NG * 2, width), preferred_element_type=f32)
    return mixed.astype(bf16)


def solution(mesh):
    finer = Mesh(mesh.devices.reshape(NY, NZ, NX, NG), BLK_GRP)
    in_specs = (
        P(BLK_GRP, None),
        P("grp", BLK),
        P("grp", BLK),
        P("grp", BLK, None),
        P("grp", BLK, None),
        P("grp", BLK, None),
    )
    return jax.shard_map(
        on_device, mesh=finer, in_specs=in_specs, out_specs=P(BLK_GRP, None), check_vma=False
    )
```

```python
import jax
import jax.numpy as jnp
import numpy as np
from jax import lax
from jax.experimental import pallas as pl
from jax.experimental.pallas import tpu as pltpu
from jax.sharding import Mesh
from jax.sharding import PartitionSpec as P

BLK = ("y", "z", "x")
BLK_GRP = ("y", "z", "x", "grp")
NY, NZ, NX = 8, 3, 4
NH, NC = 4, 2
NG = NH * NC
YC, XC = 3, 6
YR, XR = NX * NZ * 2 // YC, NY * NZ * 2 // XC
ROWS = NX * NY * NZ * 2
FAR_FIRST = [(h, c) for h in (2, 1, 3, 0) for c in range(NC) if h or c]
LEFT, RIGHT = 0, 1
LEFT_EIGHTHS = 3


def remote(src, dst, send_sem, recv_sem, **where):
    return pltpu.make_async_remote_copy(
        src_ref=src,
        dst_ref=dst,
        send_sem=send_sem,
        recv_sem=recv_sem,
        device_id=where,
        device_id_type=pl.DeviceIdType.MESH,
    )


def turn(index, by, size):
    return lax.rem(index + by + size, size)


def far_first(size):
    return sorted(range(1, size), key=lambda d: -min(d, size - d))


def each(count):
    return [(c, way) for c in range(count) for way in range(2)]


def ring_gather(go, axis, me, size, chunks, buf, sems, recvs):
    steps = size // 2
    middle = buf.shape[-1] // 2

    def copy(block, hop, way, c):
        ref = buf.at[block * chunks + c]
        if hop == steps:
            ref = ref.at[:, :middle] if way == 0 else ref.at[:, middle:]
        at = ((hop - 1) * 2 + way) * chunks + c
        return remote(ref, ref, sems.at[at], recvs.at[at], **{axis: turn(me, 1 - 2 * way, size)})

    def send(hop, way, c):
        go(copy(turn(me, (2 * way - 1) * (hop - 1), size), hop, way, c))

    def wait(hop, way, c):
        copy(turn(me, (2 * way - 1) * hop, size), hop, way, c).wait_recv()

    return send, wait


def ring_sum(go, axis, me, size, chunks, parts, buf, landed, sems, recvs):
    steps = size // 2
    half = buf.shape[-1]
    middle = half // 2
    f32, bf16 = jnp.float32, jnp.bfloat16

    def cut(ref, hop, way):
        if hop == 1:
            ref = ref.at[:, :middle] if way == 0 else ref.at[:, middle:]
        return ref

    def copy(hop, way, c):
        sign = 1 - 2 * way
        at = ((hop - 1) * 2 + way) * chunks + c
        dest = turn(me, sign * (steps + 1 - hop), size)
        return remote(
            cut(buf.at[dest * chunks + c], hop, way),
            cut(landed.at[at], hop, way),
            sems.at[at],
            recvs.at[at],
            **{axis: turn(me, sign, size)},
        )

    def first(c):
        at = turn(me, steps, size) * chunks + c
        buf[at] = parts[at].astype(bf16)
        for way in range(2):
            go(copy(1, way, c))

    def add(hop, way, c):
        copy(hop, way, c).wait_recv()
        at = turn(me, (1 - 2 * way) * (steps - hop), size) * chunks + c
        got = landed.at[((hop - 1) * 2 + way) * chunks + c]
        if hop == 1:
            mine, other = (slice(0, middle), slice(middle, half))[:: 1 - 2 * way]
            buf[at, :, mine] = (parts[at, :, mine] + got[:, mine].astype(f32)).astype(bf16)
            buf[at, :, other] = parts[at, :, other].astype(bf16)
        else:
            buf[at] = (parts[at] + got[...].astype(f32)).astype(bf16)
        go(copy(hop + 1, way, c))

    def last(c):
        total = parts[me * chunks + c]
        for way in range(2):
            copy(steps, way, c).wait_recv()
            total = total + landed[((steps - 1) * 2 + way) * chunks + c].astype(f32)
        return total

    return first, add, last


def layer_kernel(
    ids_hbm,
    gates_hbm,
    perm_hbm,
    perm_t_hbm,
    tokens_hbm,
    gate_hbm,
    up_hbm,
    down_hbm,
    out_hbm,
    ids_raw,
    gates_raw,
    perm,
    perm_t,
    ids,
    gates,
    tokens,
    w_in,
    w_out,
    all_ids,
    owned,
    cand_f32,
    cand_l,
    cand_r,
    arrived_l,
    arrived_r,
    z_rows_l,
    z_rows_r,
    x_rows,
    y_rows,
    flat_f32,
    ring_y,
    ring_x,
    part_y,
    part_x,
    sum_y,
    sum_x,
    got_y,
    got_x,
    mid_x_f32,
    mid_x,
    mid_x_got,
    mid_y_f32,
    mid_y,
    mid_y_got,
    mid_z_l,
    mid_z_r,
    mid_z_got_l,
    mid_z_got_r,
    weighted_l,
    weighted_r,
    gathered_l,
    gathered_r,
    mixed,
    w_sem,
    out_sem,
    *sems,
):
    y, z, x = lax.axis_index("y"), lax.axis_index("z"), lax.axis_index("x")
    g = lax.axis_index("grp")
    chip, core = g // NC, lax.rem(g, NC)
    tok_dev, width = tokens.shape
    hid = gate_hbm.shape[1]
    pad = w_out.shape[0]
    wide = (x_rows.shape[-1], y_rows.shape[-1])
    cols = (slice(0, wide[0]), slice(wide[0], width))
    cand, arrived = (cand_l, cand_r), (arrived_l, arrived_r)
    z_rows = (z_rows_l, z_rows_r)
    mid_z, mid_z_got = (mid_z_l, mid_z_r), (mid_z_got_l, mid_z_got_r)
    weighted, gathered = (weighted_l, weighted_r), (gathered_l, gathered_r)
    f32, bf16 = jnp.float32, jnp.bfloat16
    (
        (id_send, id_recv),
        (row_send, row_recv),
        (gz_send, gz_recv),
        (gx_send, gx_recv),
        (gy_send, gy_recv),
        ring_gy,
        ring_gx,
        ring_sy,
        ring_sx,
        (sx_send, sx_recv),
        (sy_send, sy_recv),
        (sz_send, sz_recv),
        (out_send, out_recv),
    ) = zip(sems[::2], sems[1::2])
    sent = []

    def go(copy):
        copy.start()
        sent.append(copy)

    def peer(h, c, sign=1):
        return turn(chip, sign * h, NH) * NC + turn(core, sign * c, NC)

    small = [
        pltpu.make_async_copy(src, dst, w_sem.at[n])
        for n, (src, dst) in enumerate(((ids_hbm, ids_raw), (gates_hbm, gates_raw)))
    ]
    loads = [
        pltpu.make_async_copy(src, dst, w_sem.at[n + 2])
        for n, (src, dst) in enumerate(
            (
                (tokens_hbm, tokens),
                (perm_hbm, perm),
                (perm_t_hbm, perm_t),
                (gate_hbm.at[0], w_in.at[pl.ds(0, hid)]),
                (up_hbm.at[0], w_in.at[pl.ds(pad, hid)]),
                (down_hbm.at[0], w_out.at[pl.ds(0, hid)]),
            )
        )
    ]
    barrier = pltpu.get_barrier_semaphore()
    for h, c in FAR_FIRST:
        pl.semaphore_signal(barrier, device_id={"grp": peer(h, c)})
    for o in range(1, NY):
        pl.semaphore_signal(barrier, device_id={"y": turn(y, o, NY)})
    for o in range(1, NX):
        pl.semaphore_signal(barrier, device_id={"x": turn(x, o, NX)})
    for o in range(1, NZ):
        pl.semaphore_signal(barrier, device_id={"z": turn(z, o, NZ)})
    for copy in small + loads:
        copy.start()
    for at in (hid, pad + hid):
        w_in[pl.ds(at, pad - hid), :] = jnp.zeros((pad - hid, width), bf16)
    w_out[pl.ds(hid, pad - hid), :] = jnp.zeros((pad - hid, width), bf16)
    for copy in small:
        copy.wait()
    for r in range(2):
        ids[pl.ds(r, 1), :] = jnp.broadcast_to(ids_raw[:, r : r + 1], (1, tok_dev))
        gates[pl.ds(r, 1), :] = jnp.broadcast_to(gates_raw[:, r : r + 1], (1, gates.shape[1]))
    loads[0].wait()
    pl.semaphore_wait(barrier, NG + NZ + NX + NY - 4)

    for h, c in FAR_FIRST:
        at = h * NC + c
        go(remote(ids, all_ids.at[g], id_send.at[at], id_recv.at[at], grp=peer(h, c)))
    all_ids[g] = ids[...]
    for h, c in FAR_FIRST[::-1]:
        at, landed = h * NC + c, all_ids.at[peer(h, c, -1)]
        remote(landed, landed, id_send.at[at], id_recv.at[at], grp=peer(h, c)).wait_recv()

    block = (y * NZ + z) * NX + x
    lane = lax.broadcasted_iota(jnp.int32, (2, tok_dev), 1) + (block * NG + g) * tok_dev
    for e in range(NG):
        owned[pl.ds(e * 2, 2), :] = (all_ids[e] == lane).astype(f32)
    chosen = owned[...].astype(bf16)
    for k in (RIGHT, LEFT):
        cand_f32[:, : wide[k]] = jnp.dot(chosen, tokens[:, cols[k]], preferred_element_type=f32)
        for e in range(NG):
            cand[k][e] = cand_f32[pl.ds(e * 2, 2), : wide[k]].astype(bf16)
        for h, c in FAR_FIRST:
            at, to = h * NC + c, peer(h, c)
            go(
                remote(
                    cand[k].at[to],
                    arrived[k].at[at],
                    row_send.at[k * NG + at],
                    row_recv.at[k * NG + at],
                    grp=to,
                )
            )

    def spread(k, o):
        src = z_rows[k].at[turn(z, -o, NZ)]
        axis, me, size, buf, send, recv = (
            ("x", x, NX, x_rows, gx_send, gx_recv),
            ("y", y, NY, y_rows, gy_send, gy_recv),
        )[k]
        for d in far_first(size):
            at = o * (size - 1) + d - 1
            dst = buf.at[me, turn(z, -o, NZ)]
            go(remote(src, dst, send.at[at], recv.at[at], **{axis: turn(me, d, size)}))
        buf[me, turn(z, -o, NZ)] = src[...]

    def spread_wait(k):
        axis, me, size, buf, send, recv = (
            ("x", x, NX, x_rows, gx_send, gx_recv),
            ("y", y, NY, y_rows, gy_send, gy_recv),
        )[k]
        for o in range(NZ):
            for d in range(1, size):
                at = o * (size - 1) + d - 1
                landed = buf.at[turn(me, -d, size), turn(z, -o, NZ)]
                remote(
                    landed, landed, send.at[at], recv.at[at], **{axis: turn(me, d, size)}
                ).wait_recv()

    for k in (RIGHT, LEFT):
        total = cand[k][g].astype(f32)
        for h, c in FAR_FIRST[::-1]:
            at = h * NC + c
            landed = arrived[k].at[at]
            remote(
                landed, landed, row_send.at[k * NG + at], row_recv.at[k * NG + at], grp=peer(h, c)
            ).wait_recv()
            total = total + landed[...].astype(f32)
        z_rows[k][z] = total.astype(bf16)
        for o in range(1, NZ):
            at = k * (NZ - 1) + o - 1
            ref = z_rows[k].at[z]
            go(remote(ref, ref, gz_send.at[at], gz_recv.at[at], z=turn(z, o, NZ)))
        spread(k, 0)
    for k in (RIGHT, LEFT):
        for o in range(1, NZ):
            at = k * (NZ - 1) + o - 1
            landed = z_rows[k].at[turn(z, -o, NZ)]
            remote(landed, landed, gz_send.at[at], gz_recv.at[at], z=turn(z, o, NZ)).wait_recv()
            spread(k, o)

    y_send, y_wait = ring_gather(go, "y", y, NY, YC, ring_y, *ring_gy)
    x_send, x_wait = ring_gather(go, "x", x, NX, XC, ring_x, *ring_gx)

    spread_wait(LEFT)
    for i in range(NX):
        for j in range(NZ):
            flat_f32[pl.ds((i * NZ + j) * 2, 2), : wide[LEFT]] = x_rows[i, j].astype(f32)
    for c in range(YC):
        ring_y[y * YC + c] = flat_f32[pl.ds(c * YR, YR), : wide[LEFT]].astype(bf16)
    for c, way in each(YC):
        y_send(1, way, c)
    spread_wait(RIGHT)
    for i in range(NY):
        for j in range(NZ):
            flat_f32[pl.ds((i * NZ + j) * 2, 2), :] = y_rows[i, j].astype(f32)
    for c in range(XC):
        ring_x[x * XC + c] = flat_f32[pl.ds(c * XR, XR), :].astype(bf16)
    for c, way in each(XC):
        x_send(1, way, c)
    for c, way in each(YC):
        y_wait(1, way, c)
        y_send(2, way, c)
    for c in range(max(YC, XC)):
        for way in range(2):
            if c < YC:
                y_wait(2, way, c)
                y_send(3, way, c)
            if c < XC:
                x_wait(1, way, c)
                x_send(2, way, c)
    for c, way in each(YC):
        y_wait(3, way, c)
        y_send(4, way, c)
    for copy in loads[1:]:
        copy.wait()
    for c, way in each(XC):
        x_wait(2, way, c)

    def from_ring(ref, k):
        rows = ref[...].astype(f32).reshape(ROWS, wide[k]).astype(bf16)
        return lax.dot_general(
            rows, w_in[:, cols[k]], (((1,), (1,)), ((), ())), preferred_element_type=f32
        )

    act = from_ring(ring_x, RIGHT)
    high = act.astype(bf16)
    rest = act - high.astype(f32)
    middle = rest.astype(bf16)
    low = (rest - middle.astype(f32)).astype(bf16)
    act = sum(jnp.dot(perm[...], term, preferred_element_type=f32) for term in (low, middle, high))
    for c, way in each(YC):
        y_wait(4, way, c)
    act = act + from_ring(ring_y, LEFT)
    gate_act, up_act = act[:, :pad], act[:, pad:]
    hidden = (gate_act / (1.0 + jnp.exp(-gate_act)) * up_act).astype(bf16)

    y_first, y_add, y_last = ring_sum(go, "y", y, NY, YC, part_y, sum_y, got_y, *ring_sy)
    x_first, x_add, x_last = ring_sum(go, "x", x, NX, XC, part_x, sum_x, got_x, *ring_sx)

    part_y[...] = jnp.dot(hidden, w_out[:, cols[LEFT]], preferred_element_type=f32).reshape(part_y.shape)
    for c in range(YC):
        y_first(c)
    hidden_t = jnp.dot(perm_t[...], hidden, preferred_element_type=f32).astype(bf16)
    part_x[...] = jnp.dot(hidden_t, w_out[:, cols[RIGHT]], preferred_element_type=f32).reshape(part_x.shape)
    for c in range(XC):
        x_first(c)
    for c, way in each(YC):
        y_add(1, way, c)
    for c in range(max(YC, XC)):
        for way in range(2):
            if c < YC:
                y_add(2, way, c)
            if c < XC:
                x_add(1, way, c)
    for c, way in each(YC):
        y_add(3, way, c)

    mids = (
        ("x", x, NX, mid_x_f32, mid_x, mid_x_got, sx_send, sx_recv),
        ("y", y, NY, mid_y_f32, mid_y, mid_y_got, sy_send, sy_recv),
    )

    def back(k, last, chunks, height):
        axis, me, size, exact, buf, got, send, recv = mids[k]
        for c in range(chunks):
            flat_f32[pl.ds(c * height, height), : wide[k]] = last(c)
        for i in range(size):
            for j in range(NZ):
                rows = flat_f32[pl.ds((i * NZ + j) * 2, 2), : wide[k]]
                exact[i, j] = rows
                buf[i, j] = rows.astype(bf16)
        for o in (1, 2, 0):
            for d in far_first(size):
                at = o * (size - 1) + d - 1
                src = buf.at[turn(me, d, size), turn(z, o, NZ)]
                go(remote(src, got.at[at], send.at[at], recv.at[at], **{axis: turn(me, d, size)}))

    def back_sum(k, o):
        axis, me, size, exact, buf, got, send, recv = mids[k]
        total = exact[me, turn(z, o, NZ)]
        for d in range(1, size):
            at = o * (size - 1) + d - 1
            landed = got.at[at]
            remote(
                landed, landed, send.at[at], recv.at[at], **{axis: turn(me, d, size)}
            ).wait_recv()
            total = total + landed[...].astype(f32)
        return total

    back(RIGHT, x_last, XC, XR)
    back(LEFT, y_last, YC, YR)
    for k in (LEFT, RIGHT):
        for o in range(1, NZ):
            at = k * (NZ - 1) + o - 1
            ref, landed = mid_z[k].at[o - 1], mid_z_got[k].at[o - 1]
            ref[...] = back_sum(k, o).astype(bf16)
            go(remote(ref, landed, sz_send.at[at], sz_recv.at[at], z=turn(z, o, NZ)))
    before = len(sent)
    for k in (LEFT, RIGHT):
        total = back_sum(k, 0)
        for o in range(1, NZ):
            at = k * (NZ - 1) + o - 1
            landed = mid_z_got[k].at[o - 1]
            remote(landed, landed, sz_send.at[at], sz_recv.at[at], z=turn(z, o, NZ)).wait_recv()
            total = total + landed[...].astype(f32)
        weighted[k][...] = (gates[:, :1] * total.astype(bf16).astype(f32)).astype(bf16)
        for h, c in FAR_FIRST:
            at = k * NG + h * NC + c
            go(
                remote(
                    weighted[k],
                    gathered[k].at[g],
                    out_send.at[at],
                    out_recv.at[at],
                    grp=peer(h, c),
                )
            )
        gathered[k][g] = weighted[k][...]

    for copy in sent[:before]:
        copy.wait_send()
    chosen_t = owned[...].T.astype(bf16)
    stores = []
    for k in (LEFT, RIGHT):
        for h, c in FAR_FIRST[::-1]:
            at = k * NG + h * NC + c
            landed = gathered[k].at[peer(h, c, -1)]
            remote(landed, landed, out_send.at[at], out_recv.at[at], grp=peer(h, c)).wait_recv()
        for e in range(NG):
            cand_f32[pl.ds(e * 2, 2), : wide[k]] = gathered[k][e].astype(f32)
        rows = cand_f32[:, : wide[k]].astype(bf16)
        mixed[:, cols[k]] = jnp.dot(chosen_t, rows, preferred_element_type=f32).astype(bf16)
        stores.append(
            pltpu.make_async_copy(mixed.at[:, cols[k]], out_hbm.at[:, cols[k]], out_sem.at[k])
        )
        stores[-1].start()
    for copy in sent[before:]:
        copy.wait_send()
    for copy in stores:
        copy.wait()


def swap_matrix():
    k = np.arange(ROWS)
    per = NZ * 2
    i, j, q = k // (per * NX), k // per % NX, k % per
    table = np.zeros((ROWS, ROWS), np.float32)
    table[k, (j * NY + i) * per + q] = 1
    return table


def on_device(tokens, select, gates, gate_proj, up_proj, down_proj):
    tok_dev, width = tokens.shape
    left = width * LEFT_EIGHTHS // 8
    right = width - left
    most = max(left, right)
    bf16, f32 = jnp.bfloat16, jnp.float32
    dma, vmem = pltpu.SemaphoreType.DMA, pltpu.VMEM
    hops_y, hops_x = NY * YC, NX * XC
    pad = -(-gate_proj.shape[1] // 128) * 128
    scratch = [
        vmem((1, 2), jnp.int32),
        vmem((1, 2), f32),
        vmem((ROWS, ROWS), bf16),
        vmem((ROWS, ROWS), bf16),
        vmem((2, tok_dev), jnp.int32),
        vmem((2, 128), f32),
        vmem((tok_dev, width), bf16),
        vmem((2 * pad, width), bf16),
        vmem((pad, width), bf16),
        vmem((NG, 2, tok_dev), jnp.int32),
        vmem((NG * 2, tok_dev), f32),
        vmem((NG * 2, most), f32),
        vmem((NG, 2, left), bf16),
        vmem((NG, 2, right), bf16),
        vmem((NG, 2, left), bf16),
        vmem((NG, 2, right), bf16),
        vmem((NZ, 2, left), bf16),
        vmem((NZ, 2, right), bf16),
        vmem((NX, NZ, 2, left), bf16),
        vmem((NY, NZ, 2, right), bf16),
        vmem((NY * NZ * 2, most), f32),
        vmem((NY * YC, YR, left), bf16),
        vmem((NX * XC, XR, right), bf16),
        vmem((NY * YC, YR, left), f32),
        vmem((NX * XC, XR, right), f32),
        vmem((NY * YC, YR, left), bf16),
        vmem((NX * XC, XR, right), bf16),
        vmem((hops_y, YR, left), bf16),
        vmem((hops_x, XR, right), bf16),
        vmem((NX, NZ, 2, left), f32),
        vmem((NX, NZ, 2, left), bf16),
        vmem((NZ * (NX - 1), 2, left), bf16),
        vmem((NY, NZ, 2, right), f32),
        vmem((NY, NZ, 2, right), bf16),
        vmem((NZ * (NY - 1), 2, right), bf16),
        vmem((NZ - 1, 2, left), bf16),
        vmem((NZ - 1, 2, right), bf16),
        vmem((NZ - 1, 2, left), bf16),
        vmem((NZ - 1, 2, right), bf16),
        vmem((2, left), bf16),
        vmem((2, right), bf16),
        vmem((NG, 2, left), bf16),
        vmem((NG, 2, right), bf16),
        vmem((tok_dev, width), bf16),
        dma((8,)),
        dma((2,)),
    ]
    for count in (
        NG,
        2 * NG,
        2 * (NZ - 1),
        NZ * (NX - 1),
        NZ * (NY - 1),
        hops_y,
        hops_x,
        hops_y,
        hops_x,
        NZ * (NX - 1),
        NZ * (NY - 1),
        2 * (NZ - 1),
        2 * NG,
    ):
        scratch += [dma((count,)), dma((count,))]
    in_hbm = pl.BlockSpec(memory_space=pl.ANY)
    table = swap_matrix()
    return pl.pallas_call(
        layer_kernel,
        out_shape=jax.ShapeDtypeStruct((tok_dev, width), bf16),
        in_specs=[in_hbm] * 8,
        out_specs=in_hbm,
        scratch_shapes=scratch,
        compiler_params=pltpu.CompilerParams(
            collective_id=0, has_side_effects=True, vmem_limit_bytes=56 * 1024 * 1024
        ),
        name="layer",
    )(
        select,
        gates,
        jnp.asarray(table, bf16),
        jnp.asarray(table.T, bf16),
        tokens,
        gate_proj,
        up_proj,
        down_proj,
    )


def solution(mesh):
    finer = Mesh(mesh.devices.reshape(NY, NZ, NX, NG), BLK_GRP)
    in_specs = (
        P(BLK_GRP, None),
        P("grp", BLK),
        P("grp", BLK),
        P("grp", BLK, None),
        P("grp", BLK, None),
        P("grp", BLK, None),
    )
    return jax.shard_map(
        on_device, mesh=finer, in_specs=in_specs, out_specs=P(BLK_GRP, None), check_vma=False
    )
```

```python
import jax
import jax.numpy as jnp
import numpy as np
from jax import lax
from jax.experimental import pallas as pl
from jax.experimental.pallas import tpu as pltpu
from jax.sharding import Mesh
from jax.sharding import PartitionSpec as P

BLK = ("y", "z", "x")
BLK_GRP = ("y", "z", "x", "grp")
NY, NZ, NX = 8, 3, 4
NH, NC = 4, 2
NG = NH * NC
YC, XC = 3, 6
YR, XR = NX * NZ * 2 // YC, NY * NZ * 2 // XC
ROWS = NX * NY * NZ * 2
FAR_FIRST = [(h, c) for h in (2, 1, 3, 0) for c in range(NC) if h or c]
CHIPS = (2, 1, 3)
LEFT, RIGHT = 0, 1
LEFT_EIGHTHS = 3


def remote(src, dst, send_sem, recv_sem, **where):
    return pltpu.make_async_remote_copy(
        src_ref=src,
        dst_ref=dst,
        send_sem=send_sem,
        recv_sem=recv_sem,
        device_id=where,
        device_id_type=pl.DeviceIdType.MESH,
    )


def turn(index, by, size):
    return lax.rem(index + by + size, size)


def far_first(size):
    return sorted(range(1, size), key=lambda d: -min(d, size - d))


def each(count):
    return [(c, way) for c in range(count) for way in range(2)]


def ring_gather(go, axis, me, size, chunks, buf, sems, recvs):
    steps = size // 2
    middle = buf.shape[-1] // 2

    def copy(block, hop, way, c):
        ref = buf.at[block * chunks + c]
        if hop == steps:
            ref = ref.at[:, :middle] if way == 0 else ref.at[:, middle:]
        at = ((hop - 1) * 2 + way) * chunks + c
        return remote(ref, ref, sems.at[at], recvs.at[at], **{axis: turn(me, 1 - 2 * way, size)})

    def send(hop, way, c):
        go(copy(turn(me, (2 * way - 1) * (hop - 1), size), hop, way, c))

    def wait(hop, way, c):
        copy(turn(me, (2 * way - 1) * hop, size), hop, way, c).wait_recv()

    return send, wait


def ring_sum(go, axis, me, size, chunks, parts, buf, landed, sems, recvs):
    steps = size // 2
    half = buf.shape[-1]
    middle = half // 2
    f32, bf16 = jnp.float32, jnp.bfloat16

    def cut(ref, hop, way):
        if hop == 1:
            ref = ref.at[:, :middle] if way == 0 else ref.at[:, middle:]
        return ref

    def copy(hop, way, c):
        sign = 1 - 2 * way
        at = ((hop - 1) * 2 + way) * chunks + c
        dest = turn(me, sign * (steps + 1 - hop), size)
        return remote(
            cut(buf.at[dest * chunks + c], hop, way),
            cut(landed.at[at], hop, way),
            sems.at[at],
            recvs.at[at],
            **{axis: turn(me, sign, size)},
        )

    def first(c, rows):
        buf[turn(me, steps, size) * chunks + c] = rows.astype(bf16)
        for way in range(2):
            go(copy(1, way, c))

    def add(hop, way, c):
        copy(hop, way, c).wait_recv()
        at = turn(me, (1 - 2 * way) * (steps - hop), size) * chunks + c
        got = landed.at[((hop - 1) * 2 + way) * chunks + c]
        if hop == 1:
            mine, other = (slice(0, middle), slice(middle, half))[:: 1 - 2 * way]
            buf[at, :, mine] = (parts[at, :, mine] + got[:, mine].astype(f32)).astype(bf16)
            buf[at, :, other] = parts[at, :, other].astype(bf16)
        else:
            buf[at] = (parts[at] + got[...].astype(f32)).astype(bf16)
        go(copy(hop + 1, way, c))

    def last(c):
        total = parts[me * chunks + c]
        for way in range(2):
            copy(steps, way, c).wait_recv()
            total = total + landed[((steps - 1) * 2 + way) * chunks + c].astype(f32)
        return total

    return first, add, last


def layer_kernel(
    ids_hbm,
    gates_hbm,
    perm_hbm,
    perm_t_hbm,
    tokens_hbm,
    gate_hbm,
    up_hbm,
    down_hbm,
    mixed,
    ids_raw,
    gates_raw,
    perm,
    perm_t,
    ids,
    gates,
    tokens,
    w_in,
    w_out,
    all_ids,
    owned,
    cand_f32,
    cand_l,
    cand_r,
    pair_l,
    pair_r,
    merged_l,
    merged_r,
    arrived_l,
    arrived_r,
    z_rows_l,
    z_rows_r,
    x_rows,
    y_rows,
    flat_f32,
    ring_y,
    ring_x,
    hid_y,
    hid_x,
    part_y,
    part_x,
    sum_y,
    sum_x,
    got_y,
    got_x,
    mid_x_f32,
    mid_x,
    mid_x_got,
    mid_y_f32,
    mid_y,
    mid_y_got,
    mid_z_l,
    mid_z_r,
    mid_z_got_l,
    mid_z_got_r,
    weighted_l,
    weighted_r,
    gathered_l,
    gathered_r,
    w_sem,
    *sems,
):
    y, z, x = lax.axis_index("y"), lax.axis_index("z"), lax.axis_index("x")
    g = lax.axis_index("grp")
    chip, core = g // NC, lax.rem(g, NC)
    tok_dev, width = tokens.shape
    hid = gate_hbm.shape[1]
    pad = w_out.shape[0]
    wide = (x_rows.shape[-1], y_rows.shape[-1])
    cols = (slice(0, wide[0]), slice(wide[0], width))
    cand, arrived = (cand_l, cand_r), (arrived_l, arrived_r)
    pair, merged = (pair_l, pair_r), (merged_l, merged_r)
    z_rows = (z_rows_l, z_rows_r)
    mid_z, mid_z_got = (mid_z_l, mid_z_r), (mid_z_got_l, mid_z_got_r)
    weighted, gathered = (weighted_l, weighted_r), (gathered_l, gathered_r)
    f32, bf16 = jnp.float32, jnp.bfloat16
    (
        (id_send, id_recv),
        (row_send, row_recv),
        (gz_send, gz_recv),
        (gx_send, gx_recv),
        (gy_send, gy_recv),
        ring_gy,
        ring_gx,
        ring_sy,
        ring_sx,
        (sx_send, sx_recv),
        (sy_send, sy_recv),
        (sz_send, sz_recv),
        (out_send, out_recv),
    ) = zip(sems[::2], sems[1::2])
    sent = []

    def go(copy):
        copy.start()
        sent.append(copy)

    def peer(h, c, sign=1):
        return turn(chip, sign * h, NH) * NC + turn(core, sign * c, NC)

    small = [
        pltpu.make_async_copy(src, dst, w_sem.at[n])
        for n, (src, dst) in enumerate(((ids_hbm, ids_raw), (gates_hbm, gates_raw)))
    ]
    loads = [
        pltpu.make_async_copy(src, dst, w_sem.at[n + 2])
        for n, (src, dst) in enumerate(
            (
                (tokens_hbm, tokens),
                (perm_hbm, perm),
                (perm_t_hbm, perm_t),
                (gate_hbm.at[0], w_in.at[pl.ds(0, hid)]),
                (up_hbm.at[0], w_in.at[pl.ds(pad, hid)]),
                (down_hbm.at[0], w_out.at[pl.ds(0, hid)]),
            )
        )
    ]
    barrier = pltpu.get_barrier_semaphore()
    for h, c in FAR_FIRST:
        pl.semaphore_signal(barrier, device_id={"grp": peer(h, c)})
    for o in range(1, NY):
        pl.semaphore_signal(barrier, device_id={"y": turn(y, o, NY)})
    for o in range(1, NX):
        pl.semaphore_signal(barrier, device_id={"x": turn(x, o, NX)})
    for o in range(1, NZ):
        pl.semaphore_signal(barrier, device_id={"z": turn(z, o, NZ)})
    for copy in small + loads:
        copy.start()
    for at in (hid, pad + hid):
        w_in[pl.ds(at, pad - hid), :] = jnp.zeros((pad - hid, width), bf16)
    w_out[pl.ds(hid, pad - hid), :] = jnp.zeros((pad - hid, width), bf16)
    for copy in small:
        copy.wait()
    for r in range(2):
        ids[pl.ds(r, 1), :] = jnp.broadcast_to(ids_raw[:, r : r + 1], (1, tok_dev))
        gates[pl.ds(r, 1), :] = jnp.broadcast_to(gates_raw[:, r : r + 1], (1, gates.shape[1]))
    loads[0].wait()
    pl.semaphore_wait(barrier, NG + NZ + NX + NY - 4)

    for h, c in FAR_FIRST:
        at = h * NC + c
        go(remote(ids, all_ids.at[g], id_send.at[at], id_recv.at[at], grp=peer(h, c)))
    all_ids[g] = ids[...]
    for h, c in FAR_FIRST[::-1]:
        at, landed = h * NC + c, all_ids.at[peer(h, c, -1)]
        remote(landed, landed, id_send.at[at], id_recv.at[at], grp=peer(h, c)).wait_recv()

    block = (y * NZ + z) * NX + x
    lane = lax.broadcasted_iota(jnp.int32, (2, tok_dev), 1) + (block * NG + g) * tok_dev
    for e in range(NG):
        owned[pl.ds(e * 2, 2), :] = (all_ids[e] == lane).astype(f32)
    chosen = owned[...].astype(bf16)
    for k in (RIGHT, LEFT):
        cand_f32[:, : wide[k]] = jnp.dot(chosen, tokens[:, cols[k]], preferred_element_type=f32)
        for e in range(NG):
            cand[k][e % NC, e // NC] = cand_f32[pl.ds(e * 2, 2), : wide[k]].astype(bf16)
        go(
            remote(
                cand[k].at[1 - core],
                pair[k],
                row_send.at[k * NH],
                row_recv.at[k * NH],
                grp=peer(0, 1),
            )
        )
    for k in (RIGHT, LEFT):
        remote(
            pair[k], pair[k], row_send.at[k * NH], row_recv.at[k * NH], grp=peer(0, 1)
        ).wait_recv()
        merged[k][...] = (cand[k][core].astype(f32) + pair[k][...].astype(f32)).astype(bf16)
        for h in CHIPS:
            at = k * NH + h
            go(
                remote(
                    merged[k].at[turn(chip, h, NH)],
                    arrived[k].at[h - 1],
                    row_send.at[at],
                    row_recv.at[at],
                    grp=peer(h, 0),
                )
            )

    def spread(k, o):
        src = z_rows[k].at[turn(z, -o, NZ)]
        axis, me, size, buf, send, recv = (
            ("x", x, NX, x_rows, gx_send, gx_recv),
            ("y", y, NY, y_rows, gy_send, gy_recv),
        )[k]
        for d in far_first(size):
            at = o * (size - 1) + d - 1
            dst = buf.at[me, turn(z, -o, NZ)]
            go(remote(src, dst, send.at[at], recv.at[at], **{axis: turn(me, d, size)}))
        buf[me, turn(z, -o, NZ)] = src[...]

    def spread_wait(k):
        axis, me, size, buf, send, recv = (
            ("x", x, NX, x_rows, gx_send, gx_recv),
            ("y", y, NY, y_rows, gy_send, gy_recv),
        )[k]
        for o in range(NZ):
            for d in range(1, size):
                at = o * (size - 1) + d - 1
                landed = buf.at[turn(me, -d, size), turn(z, -o, NZ)]
                remote(
                    landed, landed, send.at[at], recv.at[at], **{axis: turn(me, d, size)}
                ).wait_recv()

    for k in (RIGHT, LEFT):
        total = merged[k][chip].astype(f32)
        for h in CHIPS[::-1]:
            at, landed = k * NH + h, arrived[k].at[h - 1]
            remote(
                landed, landed, row_send.at[at], row_recv.at[at], grp=peer(h, 0)
            ).wait_recv()
            total = total + landed[...].astype(f32)
        z_rows[k][z] = total.astype(bf16)
        for o in range(1, NZ):
            at = k * (NZ - 1) + o - 1
            ref = z_rows[k].at[z]
            go(remote(ref, ref, gz_send.at[at], gz_recv.at[at], z=turn(z, o, NZ)))
        spread(k, 0)
    for k in (RIGHT, LEFT):
        for o in range(1, NZ):
            at = k * (NZ - 1) + o - 1
            landed = z_rows[k].at[turn(z, -o, NZ)]
            remote(landed, landed, gz_send.at[at], gz_recv.at[at], z=turn(z, o, NZ)).wait_recv()
            spread(k, o)

    y_send, y_wait = ring_gather(go, "y", y, NY, YC, ring_y, *ring_gy)
    x_send, x_wait = ring_gather(go, "x", x, NX, XC, ring_x, *ring_gx)

    spread_wait(LEFT)
    for i in range(NX):
        for j in range(NZ):
            flat_f32[pl.ds((i * NZ + j) * 2, 2), : wide[LEFT]] = x_rows[i, j].astype(f32)
    for c in range(YC):
        ring_y[y * YC + c] = flat_f32[pl.ds(c * YR, YR), : wide[LEFT]].astype(bf16)
    for c, way in each(YC):
        y_send(1, way, c)
    spread_wait(RIGHT)
    for i in range(NY):
        for j in range(NZ):
            flat_f32[pl.ds((i * NZ + j) * 2, 2), :] = y_rows[i, j].astype(f32)
    for c in range(XC):
        ring_x[x * XC + c] = flat_f32[pl.ds(c * XR, XR), :].astype(bf16)
    for c, way in each(XC):
        x_send(1, way, c)
    for c, way in each(YC):
        y_wait(1, way, c)
        y_send(2, way, c)
    for c in range(max(YC, XC)):
        for way in range(2):
            if c < YC:
                y_wait(2, way, c)
                y_send(3, way, c)
            if c < XC:
                x_wait(1, way, c)
                x_send(2, way, c)
    for c, way in each(YC):
        y_wait(3, way, c)
        y_send(4, way, c)
    for copy in loads[1:]:
        copy.wait()
    for c, way in each(XC):
        x_wait(2, way, c)

    def from_ring(ref, k):
        rows = ref[...].astype(f32).reshape(ROWS, wide[k]).astype(bf16)
        return lax.dot_general(
            rows, w_in[:, cols[k]], (((1,), (1,)), ((), ())), preferred_element_type=f32
        )

    act = from_ring(ring_x, RIGHT)
    high = act.astype(bf16)
    rest = act - high.astype(f32)
    middle = rest.astype(bf16)
    low = (rest - middle.astype(f32)).astype(bf16)
    act = sum(jnp.dot(perm[...], term, preferred_element_type=f32) for term in (low, middle, high))
    for c, way in each(YC):
        y_wait(4, way, c)
    act = act + from_ring(ring_y, LEFT)
    gate_act, up_act = act[:, :pad], act[:, pad:]
    hidden = gate_act / (1.0 + jnp.exp(-gate_act)) * up_act
    hid_y[...] = hidden.reshape(hid_y.shape).astype(bf16)
    hidden = hidden.astype(bf16)

    y_first, y_add, y_last = ring_sum(go, "y", y, NY, YC, part_y, sum_y, got_y, *ring_sy)
    x_first, x_add, x_last = ring_sum(go, "x", x, NX, XC, part_x, sum_x, got_x, *ring_sx)

    def down(rows, k):
        return jnp.dot(rows, w_out[:, cols[k]], preferred_element_type=f32)

    far = down(hid_y[turn(y, NY // 2, NY)], LEFT)
    for c in range(YC):
        y_first(c, far[c * YR : (c + 1) * YR])
    hidden_t = jnp.dot(perm_t[...], hidden, preferred_element_type=f32)
    hid_x[...] = hidden_t.reshape(hid_x.shape).astype(bf16)
    far = down(hid_x[turn(x, NX // 2, NX)], RIGHT)
    for c in range(XC):
        x_first(c, far[c * XR : (c + 1) * XR])
    part_y[...] = down(hidden, LEFT).reshape(part_y.shape)
    part_x[...] = down(hidden_t.astype(bf16), RIGHT).reshape(part_x.shape)
    for c, way in each(YC):
        y_add(1, way, c)
    for c in range(max(YC, XC)):
        for way in range(2):
            if c < YC:
                y_add(2, way, c)
            if c < XC:
                x_add(1, way, c)
    for c, way in each(YC):
        y_add(3, way, c)

    mids = (
        ("x", x, NX, mid_x_f32, mid_x, mid_x_got, sx_send, sx_recv),
        ("y", y, NY, mid_y_f32, mid_y, mid_y_got, sy_send, sy_recv),
    )

    def back(k, last, chunks, height):
        axis, me, size, exact, buf, got, send, recv = mids[k]
        for c in range(chunks):
            flat_f32[pl.ds(c * height, height), : wide[k]] = last(c)
        for i in range(size):
            for j in range(NZ):
                rows = flat_f32[pl.ds((i * NZ + j) * 2, 2), : wide[k]]
                exact[i, j] = rows
                buf[i, j] = rows.astype(bf16)
        for o in (1, 2, 0):
            for d in far_first(size):
                at = o * (size - 1) + d - 1
                src = buf.at[turn(me, d, size), turn(z, o, NZ)]
                go(remote(src, got.at[at], send.at[at], recv.at[at], **{axis: turn(me, d, size)}))

    def back_sum(k, o):
        axis, me, size, exact, buf, got, send, recv = mids[k]
        total = exact[me, turn(z, o, NZ)]
        for d in range(1, size):
            at = o * (size - 1) + d - 1
            landed = got.at[at]
            remote(
                landed, landed, send.at[at], recv.at[at], **{axis: turn(me, d, size)}
            ).wait_recv()
            total = total + landed[...].astype(f32)
        return total

    back(RIGHT, x_last, XC, XR)
    back(LEFT, y_last, YC, YR)
    for k in (LEFT, RIGHT):
        for o in range(1, NZ):
            at = k * (NZ - 1) + o - 1
            ref, landed = mid_z[k].at[o - 1], mid_z_got[k].at[o - 1]
            ref[...] = back_sum(k, o).astype(bf16)
            go(remote(ref, landed, sz_send.at[at], sz_recv.at[at], z=turn(z, o, NZ)))
    before = len(sent)
    for k in (LEFT, RIGHT):
        total = back_sum(k, 0)
        for o in range(1, NZ):
            at = k * (NZ - 1) + o - 1
            landed = mid_z_got[k].at[o - 1]
            remote(landed, landed, sz_send.at[at], sz_recv.at[at], z=turn(z, o, NZ)).wait_recv()
            total = total + landed[...].astype(f32)
        weighted[k][...] = (gates[:, :1] * total.astype(bf16).astype(f32)).astype(bf16)
        gathered[k][core, chip] = weighted[k][...]
        for h in CHIPS + (0,):
            at = k * 2 * NH + h
            go(
                remote(
                    weighted[k],
                    gathered[k].at[core, chip],
                    out_send.at[at],
                    out_recv.at[at],
                    grp=peer(h, 0) if h else peer(0, 1),
                )
            )

    for copy in sent[:before]:
        copy.wait_send()
    chosen_t = owned[...].T.astype(bf16)

    def landing(k, side, h):
        return gathered[k].at[side, turn(chip, -h, NH)]

    for k in (LEFT, RIGHT):
        for h in CHIPS[::-1]:
            at, ref = k * 2 * NH + h, landing(k, core, h)
            remote(ref, ref, out_send.at[at], out_recv.at[at], grp=peer(h, 0)).wait_recv()
            go(remote(ref, ref, out_send.at[at + NH], out_recv.at[at + NH], grp=peer(0, 1)))
    for k in (LEFT, RIGHT):
        for h in (0,) + CHIPS[::-1]:
            at, ref = k * 2 * NH + h + (NH if h else 0), landing(k, 1 - core, h)
            remote(ref, ref, out_send.at[at], out_recv.at[at], grp=peer(0, 1)).wait_recv()
        for e in range(NG):
            cand_f32[pl.ds(e * 2, 2), : wide[k]] = gathered[k][e % NC, e // NC].astype(f32)
        rows = cand_f32[:, : wide[k]].astype(bf16)
        mixed[:, cols[k]] = jnp.dot(chosen_t, rows, preferred_element_type=f32).astype(bf16)
    for copy in sent[before:]:
        copy.wait_send()


def swap_matrix():
    k = np.arange(ROWS)
    per = NZ * 2
    i, j, q = k // (per * NX), k // per % NX, k % per
    table = np.zeros((ROWS, ROWS), np.float32)
    table[k, (j * NY + i) * per + q] = 1
    return table


def on_device(tokens, select, gates, gate_proj, up_proj, down_proj):
    tok_dev, width = tokens.shape
    left = width * LEFT_EIGHTHS // 8
    right = width - left
    most = max(left, right)
    bf16, f32 = jnp.bfloat16, jnp.float32
    dma, vmem = pltpu.SemaphoreType.DMA, pltpu.VMEM
    hops_y, hops_x = NY * YC, NX * XC
    pad = -(-gate_proj.shape[1] // 128) * 128
    scratch = [
        vmem((1, 2), jnp.int32),
        vmem((1, 2), f32),
        vmem((ROWS, ROWS), bf16),
        vmem((ROWS, ROWS), bf16),
        vmem((2, tok_dev), jnp.int32),
        vmem((2, 128), f32),
        vmem((tok_dev, width), bf16),
        vmem((2 * pad, width), bf16),
        vmem((pad, width), bf16),
        vmem((NG, 2, tok_dev), jnp.int32),
        vmem((NG * 2, tok_dev), f32),
        vmem((NG * 2, most), f32),
        vmem((NC, NH, 2, left), bf16),
        vmem((NC, NH, 2, right), bf16),
        vmem((NH, 2, left), bf16),
        vmem((NH, 2, right), bf16),
        vmem((NH, 2, left), bf16),
        vmem((NH, 2, right), bf16),
        vmem((NH - 1, 2, left), bf16),
        vmem((NH - 1, 2, right), bf16),
        vmem((NZ, 2, left), bf16),
        vmem((NZ, 2, right), bf16),
        vmem((NX, NZ, 2, left), bf16),
        vmem((NY, NZ, 2, right), bf16),
        vmem((NY * NZ * 2, most), f32),
        vmem((NY * YC, YR, left), bf16),
        vmem((NX * XC, XR, right), bf16),
        vmem((NY, YC * YR, pad), bf16),
        vmem((NX, XC * XR, pad), bf16),
        vmem((NY * YC, YR, left), f32),
        vmem((NX * XC, XR, right), f32),
        vmem((NY * YC, YR, left), bf16),
        vmem((NX * XC, XR, right), bf16),
        vmem((hops_y, YR, left), bf16),
        vmem((hops_x, XR, right), bf16),
        vmem((NX, NZ, 2, left), f32),
        vmem((NX, NZ, 2, left), bf16),
        vmem((NZ * (NX - 1), 2, left), bf16),
        vmem((NY, NZ, 2, right), f32),
        vmem((NY, NZ, 2, right), bf16),
        vmem((NZ * (NY - 1), 2, right), bf16),
        vmem((NZ - 1, 2, left), bf16),
        vmem((NZ - 1, 2, right), bf16),
        vmem((NZ - 1, 2, left), bf16),
        vmem((NZ - 1, 2, right), bf16),
        vmem((2, left), bf16),
        vmem((2, right), bf16),
        vmem((NC, NH, 2, left), bf16),
        vmem((NC, NH, 2, right), bf16),
        dma((8,)),
    ]
    for count in (
        NG,
        2 * NH,
        2 * (NZ - 1),
        NZ * (NX - 1),
        NZ * (NY - 1),
        hops_y,
        hops_x,
        hops_y,
        hops_x,
        NZ * (NX - 1),
        NZ * (NY - 1),
        2 * (NZ - 1),
        4 * NH,
    ):
        scratch += [dma((count,)), dma((count,))]
    in_hbm = pl.BlockSpec(memory_space=pltpu.HBM)
    table = swap_matrix()
    arrays = (
        select,
        gates,
        jnp.asarray(table, bf16),
        jnp.asarray(table.T, bf16),
        tokens,
        gate_proj,
        up_proj,
        down_proj,
    )
    return pl.pallas_call(
        layer_kernel,
        out_shape=jax.ShapeDtypeStruct((tok_dev, width), bf16),
        in_specs=[in_hbm] * 8,
        out_specs=pl.BlockSpec(memory_space=pltpu.VMEM),
        scratch_shapes=scratch,
        compiler_params=pltpu.CompilerParams(
            collective_id=0, has_side_effects=True, vmem_limit_bytes=28 * 1024 * 1024
        ),
        name="layer",
    )(*(pltpu.with_memory_space_constraint(a, pltpu.HBM) for a in arrays))


def solution(mesh):
    finer = Mesh(mesh.devices.reshape(NY, NZ, NX, NG), BLK_GRP)
    in_specs = (
        P(BLK_GRP, None),
        P("grp", BLK),
        P("grp", BLK),
        P("grp", BLK, None),
        P("grp", BLK, None),
        P("grp", BLK, None),
    )
    return jax.shard_map(
        on_device, mesh=finer, in_specs=in_specs, out_specs=P(BLK_GRP, None), check_vma=False
    )
```

```python
import jax
import jax.numpy as jnp
import numpy as np
from jax import lax
from jax.experimental import pallas as pl
from jax.experimental.pallas import tpu as pltpu
from jax.sharding import Mesh
from jax.sharding import PartitionSpec as P

BLK = ("y", "z", "x")
BLK_GRP = ("y", "z", "x", "grp")
NY, NZ, NX = 8, 3, 4
NH, NC = 4, 2
NG = NH * NC
YC, XC = 3, 6
YR, XR = NX * NZ * 2 // YC, NY * NZ * 2 // XC
ROWS = NX * NY * NZ * 2
FAR_FIRST = [(h, c) for h in (2, 1, 3, 0) for c in range(NC) if h or c]
CHIPS = (2, 1, 3)
LEFT, RIGHT = 0, 1
LEFT_EIGHTHS = 3


def remote(src, dst, send_sem, recv_sem, **where):
    return pltpu.make_async_remote_copy(
        src_ref=src,
        dst_ref=dst,
        send_sem=send_sem,
        recv_sem=recv_sem,
        device_id=where,
        device_id_type=pl.DeviceIdType.MESH,
    )


def turn(index, by, size):
    return lax.rem(index + by + size, size)


def far_first(size):
    return sorted(range(1, size), key=lambda d: -min(d, size - d))


def each(count):
    return [(c, way) for c in range(count) for way in range(2)]


def ring_gather(go, axis, me, size, chunks, buf, sems, recvs):
    steps = size // 2
    middle = buf.shape[-1] // 2

    def copy(block, hop, way, c):
        ref = buf.at[block * chunks + c]
        if hop == steps:
            ref = ref.at[:, :middle] if way == 0 else ref.at[:, middle:]
        at = ((hop - 1) * 2 + way) * chunks + c
        return remote(ref, ref, sems.at[at], recvs.at[at], **{axis: turn(me, 1 - 2 * way, size)})

    def send(hop, way, c):
        go(copy(turn(me, (2 * way - 1) * (hop - 1), size), hop, way, c))

    def wait(hop, way, c):
        copy(turn(me, (2 * way - 1) * hop, size), hop, way, c).wait_recv()

    return send, wait


def ring_sum(go, axis, me, size, chunks, parts, buf, landed, sems, recvs):
    steps = size // 2
    half = buf.shape[-1]
    middle = half // 2
    f32, bf16 = jnp.float32, jnp.bfloat16

    def cut(ref, hop, way):
        if hop == 1:
            ref = ref.at[:, :middle] if way == 0 else ref.at[:, middle:]
        return ref

    def copy(hop, way, c):
        sign = 1 - 2 * way
        at = ((hop - 1) * 2 + way) * chunks + c
        dest = turn(me, sign * (steps + 1 - hop), size)
        return remote(
            cut(buf.at[dest * chunks + c], hop, way),
            cut(landed.at[at], hop, way),
            sems.at[at],
            recvs.at[at],
            **{axis: turn(me, sign, size)},
        )

    def first(c, rows):
        buf[turn(me, steps, size) * chunks + c] = rows.astype(bf16)
        for way in range(2):
            go(copy(1, way, c))

    def add(hop, way, c):
        copy(hop, way, c).wait_recv()
        at = turn(me, (1 - 2 * way) * (steps - hop), size) * chunks + c
        got = landed.at[((hop - 1) * 2 + way) * chunks + c]
        if hop == 1:
            mine, other = (slice(0, middle), slice(middle, half))[:: 1 - 2 * way]
            buf[at, :, mine] = (parts[at, :, mine] + got[:, mine].astype(f32)).astype(bf16)
            buf[at, :, other] = parts[at, :, other].astype(bf16)
        else:
            buf[at] = (parts[at] + got[...].astype(f32)).astype(bf16)
        go(copy(hop + 1, way, c))

    def last(c):
        total = parts[me * chunks + c]
        for way in range(2):
            copy(steps, way, c).wait_recv()
            total = total + landed[((steps - 1) * 2 + way) * chunks + c].astype(f32)
        return total

    return first, add, last


def layer_kernel(
    ids_hbm,
    gates_hbm,
    perm_hbm,
    perm_t_hbm,
    tokens_hbm,
    gate_hbm,
    up_hbm,
    down_hbm,
    mixed,
    ids_raw,
    gates_raw,
    perm,
    perm_t,
    ids,
    gates,
    tokens,
    w_in,
    w_out,
    all_ids,
    owned,
    cand_f32,
    cand_l,
    cand_r,
    pair_l,
    pair_r,
    merged_l,
    merged_r,
    arrived_l,
    arrived_r,
    z_rows_l,
    z_rows_r,
    x_rows,
    y_rows,
    flat_f32,
    ring_y,
    ring_x,
    hid_y,
    hid_x,
    part_y,
    part_x,
    sum_y,
    sum_x,
    got_y,
    got_x,
    mid_x_f32,
    mid_x,
    mid_x_got,
    mid_y_f32,
    mid_y,
    mid_y_got,
    mid_z_l,
    mid_z_r,
    mid_z_got_l,
    mid_z_got_r,
    weighted_l,
    weighted_r,
    gathered_l,
    gathered_r,
    w_sem,
    *sems,
):
    y, z, x = lax.axis_index("y"), lax.axis_index("z"), lax.axis_index("x")
    g = lax.axis_index("grp")
    chip, core = g // NC, lax.rem(g, NC)
    tok_dev, width = tokens.shape
    hid = gate_hbm.shape[1]
    pad = w_out.shape[0]
    wide = (x_rows.shape[-1], y_rows.shape[-1])
    cols = (slice(0, wide[0]), slice(wide[0], width))
    cand, arrived = (cand_l, cand_r), (arrived_l, arrived_r)
    pair, merged = (pair_l, pair_r), (merged_l, merged_r)
    z_rows = (z_rows_l, z_rows_r)
    mid_z, mid_z_got = (mid_z_l, mid_z_r), (mid_z_got_l, mid_z_got_r)
    weighted, gathered = (weighted_l, weighted_r), (gathered_l, gathered_r)
    f32, bf16 = jnp.float32, jnp.bfloat16
    (
        (id_send, id_recv),
        (row_send, row_recv),
        (gz_send, gz_recv),
        (gx_send, gx_recv),
        (gy_send, gy_recv),
        ring_gy,
        ring_gx,
        ring_sy,
        ring_sx,
        (sx_send, sx_recv),
        (sy_send, sy_recv),
        (sz_send, sz_recv),
        (out_send, out_recv),
    ) = zip(sems[::2], sems[1::2])
    sent = []

    def go(copy):
        copy.start()
        sent.append(copy)

    def peer(h, c, sign=1):
        return turn(chip, sign * h, NH) * NC + turn(core, sign * c, NC)

    small = [
        pltpu.make_async_copy(src, dst, w_sem.at[n])
        for n, (src, dst) in enumerate(((ids_hbm, ids_raw), (gates_hbm, gates_raw)))
    ]
    loads = [
        pltpu.make_async_copy(src, dst, w_sem.at[n + 2])
        for n, (src, dst) in enumerate(
            (
                (tokens_hbm, tokens),
                (perm_hbm, perm),
                (perm_t_hbm, perm_t),
                (gate_hbm.at[0], w_in.at[pl.ds(0, hid)]),
                (up_hbm.at[0], w_in.at[pl.ds(pad, hid)]),
                (down_hbm.at[0], w_out.at[pl.ds(0, hid)]),
            )
        )
    ]
    barrier = pltpu.get_barrier_semaphore()
    for h, c in FAR_FIRST:
        pl.semaphore_signal(barrier, device_id={"grp": peer(h, c)})
    for o in range(1, NY):
        pl.semaphore_signal(barrier, device_id={"y": turn(y, o, NY)})
    for o in range(1, NX):
        pl.semaphore_signal(barrier, device_id={"x": turn(x, o, NX)})
    for o in range(1, NZ):
        pl.semaphore_signal(barrier, device_id={"z": turn(z, o, NZ)})
    for copy in small + loads:
        copy.start()
    for at in (hid, pad + hid):
        w_in[pl.ds(at, pad - hid), :] = jnp.zeros((pad - hid, width), bf16)
    w_out[pl.ds(hid, pad - hid), :] = jnp.zeros((pad - hid, width), bf16)
    for copy in small:
        copy.wait()
    for r in range(2):
        ids[pl.ds(r, 1), :] = jnp.broadcast_to(ids_raw[:, r : r + 1], (1, tok_dev))
        gates[pl.ds(r, 1), :] = jnp.broadcast_to(gates_raw[:, r : r + 1], (1, gates.shape[1]))
    loads[0].wait()
    pl.semaphore_wait(barrier, NG + NZ + NX + NY - 4)

    for h, c in FAR_FIRST:
        at = h * NC + c
        go(remote(ids, all_ids.at[g], id_send.at[at], id_recv.at[at], grp=peer(h, c)))
    all_ids[g] = ids[...]
    for h, c in FAR_FIRST[::-1]:
        at, landed = h * NC + c, all_ids.at[peer(h, c, -1)]
        remote(landed, landed, id_send.at[at], id_recv.at[at], grp=peer(h, c)).wait_recv()

    block = (y * NZ + z) * NX + x
    lane = lax.broadcasted_iota(jnp.int32, (2, tok_dev), 1) + (block * NG + g) * tok_dev
    for e in range(NG):
        owned[pl.ds(e * 2, 2), :] = (all_ids[e] == lane).astype(f32)
    chosen = owned[...].astype(bf16)
    for k in (RIGHT, LEFT):
        cand_f32[:, : wide[k]] = jnp.dot(chosen, tokens[:, cols[k]], preferred_element_type=f32)
        for e in range(NG):
            cand[k][e % NC, e // NC] = cand_f32[pl.ds(e * 2, 2), : wide[k]].astype(bf16)
        go(
            remote(
                cand[k].at[1 - core],
                pair[k],
                row_send.at[k * NH],
                row_recv.at[k * NH],
                grp=peer(0, 1),
            )
        )
    for k in (RIGHT, LEFT):
        remote(
            pair[k], pair[k], row_send.at[k * NH], row_recv.at[k * NH], grp=peer(0, 1)
        ).wait_recv()
        merged[k][...] = (cand[k][core].astype(f32) + pair[k][...].astype(f32)).astype(bf16)
        for h in CHIPS:
            at = k * NH + h
            go(
                remote(
                    merged[k].at[turn(chip, h, NH)],
                    arrived[k].at[h - 1],
                    row_send.at[at],
                    row_recv.at[at],
                    grp=peer(h, 0),
                )
            )

    def spread(k, o):
        src = z_rows[k].at[turn(z, -o, NZ)]
        axis, me, size, buf, send, recv = (
            ("x", x, NX, x_rows, gx_send, gx_recv),
            ("y", y, NY, y_rows, gy_send, gy_recv),
        )[k]
        for d in far_first(size):
            at = o * (size - 1) + d - 1
            dst = buf.at[me, turn(z, -o, NZ)]
            go(remote(src, dst, send.at[at], recv.at[at], **{axis: turn(me, d, size)}))
        buf[me, turn(z, -o, NZ)] = src[...]

    def spread_wait(k):
        axis, me, size, buf, send, recv = (
            ("x", x, NX, x_rows, gx_send, gx_recv),
            ("y", y, NY, y_rows, gy_send, gy_recv),
        )[k]
        for o in range(NZ):
            for d in range(1, size):
                at = o * (size - 1) + d - 1
                landed = buf.at[turn(me, -d, size), turn(z, -o, NZ)]
                remote(
                    landed, landed, send.at[at], recv.at[at], **{axis: turn(me, d, size)}
                ).wait_recv()

    for k in (RIGHT, LEFT):
        total = merged[k][chip].astype(f32)
        for h in CHIPS[::-1]:
            at, landed = k * NH + h, arrived[k].at[h - 1]
            remote(
                landed, landed, row_send.at[at], row_recv.at[at], grp=peer(h, 0)
            ).wait_recv()
            total = total + landed[...].astype(f32)
        z_rows[k][z] = total.astype(bf16)
        for o in range(1, NZ):
            at = k * (NZ - 1) + o - 1
            ref = z_rows[k].at[z]
            go(remote(ref, ref, gz_send.at[at], gz_recv.at[at], z=turn(z, o, NZ)))
        spread(k, 0)
    for k in (RIGHT, LEFT):
        for o in range(1, NZ):
            at = k * (NZ - 1) + o - 1
            landed = z_rows[k].at[turn(z, -o, NZ)]
            remote(landed, landed, gz_send.at[at], gz_recv.at[at], z=turn(z, o, NZ)).wait_recv()
            spread(k, o)

    y_send, y_wait = ring_gather(go, "y", y, NY, YC, ring_y, *ring_gy)
    x_send, x_wait = ring_gather(go, "x", x, NX, XC, ring_x, *ring_gx)

    spread_wait(LEFT)
    for c in range(YC):
        for p in range(c * YR // 2, (c + 1) * YR // 2):
            flat_f32[pl.ds(p * 2, 2), : wide[LEFT]] = x_rows[p // NZ, p % NZ].astype(f32)
        ring_y[y * YC + c] = flat_f32[pl.ds(c * YR, YR), : wide[LEFT]].astype(bf16)
        for way in range(2):
            y_send(1, way, c)
    spread_wait(RIGHT)
    for c in range(XC):
        for p in range(c * XR // 2, (c + 1) * XR // 2):
            flat_f32[pl.ds(p * 2, 2), : wide[RIGHT]] = y_rows[p // NZ, p % NZ].astype(f32)
        ring_x[x * XC + c] = flat_f32[pl.ds(c * XR, XR), : wide[RIGHT]].astype(bf16)
        for way in range(2):
            x_send(1, way, c)
    for c, way in each(YC):
        y_wait(1, way, c)
        y_send(2, way, c)
    for c in range(max(YC, XC)):
        for way in range(2):
            if c < YC:
                y_wait(2, way, c)
                y_send(3, way, c)
            if c < XC:
                x_wait(1, way, c)
                x_send(2, way, c)
    for c, way in each(YC):
        y_wait(3, way, c)
        y_send(4, way, c)
    for copy in loads[1:]:
        copy.wait()
    for c, way in each(XC):
        x_wait(2, way, c)

    def from_ring(ref, k):
        rows = ref[...].astype(f32).reshape(ROWS, wide[k]).astype(bf16)
        return lax.dot_general(
            rows, w_in[:, cols[k]], (((1,), (1,)), ((), ())), preferred_element_type=f32
        )

    act = from_ring(ring_x, RIGHT)
    high = act.astype(bf16)
    rest = act - high.astype(f32)
    middle = rest.astype(bf16)
    low = (rest - middle.astype(f32)).astype(bf16)
    act = sum(jnp.dot(perm[...], term, preferred_element_type=f32) for term in (low, middle, high))
    for c, way in each(YC):
        y_wait(4, way, c)
    act = act + from_ring(ring_y, LEFT)
    gate_act, up_act = act[:, :pad], act[:, pad:]
    hidden = gate_act / (1.0 + jnp.exp(-gate_act)) * up_act
    hid_y[...] = hidden.reshape(hid_y.shape).astype(bf16)
    hidden = hidden.astype(bf16)

    y_first, y_add, y_last = ring_sum(go, "y", y, NY, YC, part_y, sum_y, got_y, *ring_sy)
    x_first, x_add, x_last = ring_sum(go, "x", x, NX, XC, part_x, sum_x, got_x, *ring_sx)

    def down(rows, k):
        return jnp.dot(rows, w_out[:, cols[k]], preferred_element_type=f32)

    far = down(hid_y[turn(y, NY // 2, NY)], LEFT)
    for c in range(YC):
        y_first(c, far[c * YR : (c + 1) * YR])
    hidden_t = jnp.dot(perm_t[...], hidden, preferred_element_type=f32)
    hid_x[...] = hidden_t.reshape(hid_x.shape).astype(bf16)
    far = down(hid_x[turn(x, NX // 2, NX)], RIGHT)
    for c in range(XC):
        x_first(c, far[c * XR : (c + 1) * XR])
    part_y[...] = down(hidden, LEFT).reshape(part_y.shape)
    part_x[...] = down(hidden_t.astype(bf16), RIGHT).reshape(part_x.shape)
    for c, way in each(YC):
        y_add(1, way, c)
    for c in range(max(YC, XC)):
        for way in range(2):
            if c < YC:
                y_add(2, way, c)
            if c < XC:
                x_add(1, way, c)
    for c, way in each(YC):
        y_add(3, way, c)

    mids = (
        ("x", x, NX, mid_x_f32, mid_x, mid_x_got, sx_send, sx_recv),
        ("y", y, NY, mid_y_f32, mid_y, mid_y_got, sy_send, sy_recv),
    )

    def back(k, last, chunks, height):
        axis, me, size, exact, buf, got, send, recv = mids[k]
        for c in range(chunks):
            flat_f32[pl.ds(c * height, height), : wide[k]] = last(c)
            for first in range(c * height, (c + 1) * height, 2):
                rows = flat_f32[pl.ds(first, 2), : wide[k]]
                i, j = first // 2 // NZ, first // 2 % NZ
                exact[i, j] = rows
                buf[i, j] = rows.astype(bf16)
        for o in (1, 2, 0):
            for d in far_first(size):
                at = o * (size - 1) + d - 1
                src = buf.at[turn(me, d, size), turn(z, o, NZ)]
                go(remote(src, got.at[at], send.at[at], recv.at[at], **{axis: turn(me, d, size)}))

    def back_sum(k, o):
        axis, me, size, exact, buf, got, send, recv = mids[k]
        total = exact[me, turn(z, o, NZ)]
        for d in range(1, size):
            at = o * (size - 1) + d - 1
            landed = got.at[at]
            remote(
                landed, landed, send.at[at], recv.at[at], **{axis: turn(me, d, size)}
            ).wait_recv()
            total = total + landed[...].astype(f32)
        return total

    back(RIGHT, x_last, XC, XR)
    back(LEFT, y_last, YC, YR)
    for k in (LEFT, RIGHT):
        for o in range(1, NZ):
            at = k * (NZ - 1) + o - 1
            ref, landed = mid_z[k].at[o - 1], mid_z_got[k].at[o - 1]
            ref[...] = back_sum(k, o).astype(bf16)
            go(remote(ref, landed, sz_send.at[at], sz_recv.at[at], z=turn(z, o, NZ)))
    before = len(sent)
    for k in (LEFT, RIGHT):
        total = back_sum(k, 0)
        for o in range(1, NZ):
            at = k * (NZ - 1) + o - 1
            landed = mid_z_got[k].at[o - 1]
            remote(landed, landed, sz_send.at[at], sz_recv.at[at], z=turn(z, o, NZ)).wait_recv()
            total = total + landed[...].astype(f32)
        weighted[k][...] = (gates[:, :1] * total.astype(bf16).astype(f32)).astype(bf16)
        gathered[k][core, chip] = weighted[k][...]
        for h in CHIPS + (0,):
            at = k * 2 * NH + h
            go(
                remote(
                    weighted[k],
                    gathered[k].at[core, chip],
                    out_send.at[at],
                    out_recv.at[at],
                    grp=peer(h, 0) if h else peer(0, 1),
                )
            )

    for copy in sent[:before]:
        copy.wait_send()
    chosen_t = owned[...].T.astype(bf16)

    def landing(k, side, h):
        return gathered[k].at[side, turn(chip, -h, NH)]

    for k in (LEFT, RIGHT):
        for h in CHIPS[::-1]:
            at, ref = k * 2 * NH + h, landing(k, core, h)
            remote(ref, ref, out_send.at[at], out_recv.at[at], grp=peer(h, 0)).wait_recv()
            go(remote(ref, ref, out_send.at[at + NH], out_recv.at[at + NH], grp=peer(0, 1)))
    for k in (LEFT, RIGHT):
        for h in (0,) + CHIPS[::-1]:
            at, ref = k * 2 * NH + h + (NH if h else 0), landing(k, 1 - core, h)
            remote(ref, ref, out_send.at[at], out_recv.at[at], grp=peer(0, 1)).wait_recv()
        for e in range(NG):
            cand_f32[pl.ds(e * 2, 2), : wide[k]] = gathered[k][e % NC, e // NC].astype(f32)
        rows = cand_f32[:, : wide[k]].astype(bf16)
        mixed[:, cols[k]] = jnp.dot(chosen_t, rows, preferred_element_type=f32).astype(bf16)
    for copy in sent[before:]:
        copy.wait_send()


def swap_matrix():
    k = np.arange(ROWS)
    per = NZ * 2
    i, j, q = k // (per * NX), k // per % NX, k % per
    table = np.zeros((ROWS, ROWS), np.float32)
    table[k, (j * NY + i) * per + q] = 1
    return table


def on_device(tokens, select, gates, gate_proj, up_proj, down_proj):
    tok_dev, width = tokens.shape
    left = width * LEFT_EIGHTHS // 8
    right = width - left
    most = max(left, right)
    bf16, f32 = jnp.bfloat16, jnp.float32
    dma, vmem = pltpu.SemaphoreType.DMA, pltpu.VMEM
    hops_y, hops_x = NY * YC, NX * XC
    pad = -(-gate_proj.shape[1] // 128) * 128
    scratch = [
        vmem((1, 2), jnp.int32),
        vmem((1, 2), f32),
        vmem((ROWS, ROWS), bf16),
        vmem((ROWS, ROWS), bf16),
        vmem((2, tok_dev), jnp.int32),
        vmem((2, 128), f32),
        vmem((tok_dev, width), bf16),
        vmem((2 * pad, width), bf16),
        vmem((pad, width), bf16),
        vmem((NG, 2, tok_dev), jnp.int32),
        vmem((NG * 2, tok_dev), f32),
        vmem((NG * 2, most), f32),
        vmem((NC, NH, 2, left), bf16),
        vmem((NC, NH, 2, right), bf16),
        vmem((NH, 2, left), bf16),
        vmem((NH, 2, right), bf16),
        vmem((NH, 2, left), bf16),
        vmem((NH, 2, right), bf16),
        vmem((NH - 1, 2, left), bf16),
        vmem((NH - 1, 2, right), bf16),
        vmem((NZ, 2, left), bf16),
        vmem((NZ, 2, right), bf16),
        vmem((NX, NZ, 2, left), bf16),
        vmem((NY, NZ, 2, right), bf16),
        vmem((NY * NZ * 2, most), f32),
        vmem((NY * YC, YR, left), bf16),
        vmem((NX * XC, XR, right), bf16),
        vmem((NY, YC * YR, pad), bf16),
        vmem((NX, XC * XR, pad), bf16),
        vmem((NY * YC, YR, left), f32),
        vmem((NX * XC, XR, right), f32),
        vmem((NY * YC, YR, left), bf16),
        vmem((NX * XC, XR, right), bf16),
        vmem((hops_y, YR, left), bf16),
        vmem((hops_x, XR, right), bf16),
        vmem((NX, NZ, 2, left), f32),
        vmem((NX, NZ, 2, left), bf16),
        vmem((NZ * (NX - 1), 2, left), bf16),
        vmem((NY, NZ, 2, right), f32),
        vmem((NY, NZ, 2, right), bf16),
        vmem((NZ * (NY - 1), 2, right), bf16),
        vmem((NZ - 1, 2, left), bf16),
        vmem((NZ - 1, 2, right), bf16),
        vmem((NZ - 1, 2, left), bf16),
        vmem((NZ - 1, 2, right), bf16),
        vmem((2, left), bf16),
        vmem((2, right), bf16),
        vmem((NC, NH, 2, left), bf16),
        vmem((NC, NH, 2, right), bf16),
        dma((8,)),
    ]
    for count in (
        NG,
        2 * NH,
        2 * (NZ - 1),
        NZ * (NX - 1),
        NZ * (NY - 1),
        hops_y,
        hops_x,
        hops_y,
        hops_x,
        NZ * (NX - 1),
        NZ * (NY - 1),
        2 * (NZ - 1),
        4 * NH,
    ):
        scratch += [dma((count,)), dma((count,))]
    in_hbm = pl.BlockSpec(memory_space=pltpu.HBM)
    table = swap_matrix()
    arrays = (
        select,
        gates,
        jnp.asarray(table, bf16),
        jnp.asarray(table.T, bf16),
        tokens,
        gate_proj,
        up_proj,
        down_proj,
    )
    return pl.pallas_call(
        layer_kernel,
        out_shape=jax.ShapeDtypeStruct((tok_dev, width), bf16),
        in_specs=[in_hbm] * 8,
        out_specs=pl.BlockSpec(memory_space=pltpu.VMEM),
        scratch_shapes=scratch,
        compiler_params=pltpu.CompilerParams(
            collective_id=0, has_side_effects=True, vmem_limit_bytes=28 * 1024 * 1024
        ),
        name="layer",
    )(*(pltpu.with_memory_space_constraint(a, pltpu.HBM) for a in arrays))


def solution(mesh):
    finer = Mesh(mesh.devices.reshape(NY, NZ, NX, NG), BLK_GRP)
    in_specs = (
        P(BLK_GRP, None),
        P("grp", BLK),
        P("grp", BLK),
        P("grp", BLK, None),
        P("grp", BLK, None),
        P("grp", BLK, None),
    )
    return jax.shard_map(
        on_device, mesh=finer, in_specs=in_specs, out_specs=P(BLK_GRP, None), check_vma=False
    )
```
